256 devices in a mesh: seq: 128 (over x_lo, y, z, core), batch: 2 (over x_hi).
Axes of the slice: x: 4 (x_hi: 2, x_lo: 2; x = x_hi * 2 + x_lo), y: 4, z: 8, core: 2. Of those that a mesh axis runs over, the one named last changes fastest.
Arguments:
- hidden_in: bfloat16 [2, 32768, 2304], P('batch', 'seq'), may hold values from -6 to 6
- segment_ids: int32 [2, 32768], P('batch', 'seq'), may hold values from 0 to 15, never falling along the last dimension, each value on 1 to 4096 neighbouring positions
- pre_gain: float32 [2304], replicated, may hold values from 0.25 to 1.75
- w_qkv: bfloat16 [2304, 2048], P('seq'), may hold values from -0.27083333 to 0.27083333
- w_out: bfloat16 [1024, 2304], P('seq'), may hold values from -0.1875 to 0.1875
- post_gain: float32 [2304], replicated, may hold values from 0.25 to 1.75
Outputs:
- layer_out: bfloat16 [2, 32768, 2304], P('batch', 'seq')
The draws below stay inside these ranges and needn't reach their ends.
Inputs may be any that keep to these rules, and one draw needn't show every extreme that they name: `segment_ids`: along each sequence the numbers never fall; a document is 1 to 4096 positions long, and each sequence has one of exactly 4096.
All inputs are finite; a program needn't handle non-finite values.
Results may differ from the reference program's by a relative error of at most 0.012.
The reference program's roundings to bfloat16 on the way (of `normed` and `attended`) count: a program that leaves them out, or rounds other values in their place, can miss the bound.
Values may be sent and summed in bfloat16 or wider, within the bound.
A program may use at most 128 MiB of HBM per device.

```python
import math
import jax
import jax.numpy as jnp
import numpy as np
from jax import lax

D = 2304
Q_HEADS = 4
KV_HEADS = 2
HEAD = 256
WINDOW = 4096
DOCS = 16
TOK_DEV = 256
SEQ = 32768
BATCH = 2
QKV_W = 2048
ATT_W = 1024
DOC_MOST = 4096


def draw_w_qkv(key, part):
    base_key = jax.random.fold_in(key, 11)
    pick_key = jax.random.fold_in(key, 12)
    base = jnp.clip(jax.random.normal(base_key, (D, QKV_W), jnp.float32), -3.0, 3.0)
    order = jax.random.permutation(pick_key, KV_HEADS)
    boosted = order < (KV_HEADS + 1) // 2
    columns = jnp.arange(QKV_W, dtype=jnp.int32)
    head_of = columns // HEAD
    group_of = jnp.where(head_of < Q_HEADS, head_of // (Q_HEADS // KV_HEADS), head_of - Q_HEADS)
    group_of = jnp.clip(group_of, 0, KV_HEADS - 1)
    is_value = head_of >= Q_HEADS + KV_HEADS
    factor = jnp.where(boosted[group_of] & jnp.logical_not(is_value), 4.0, 1.0).astype(jnp.float32)
    return (base * factor[None, :] * float(D) ** (-0.5)).astype(jnp.bfloat16)


def block_levels(stream_key, dims, cuts, least, high):
    def one(position, shards_of):
        steps = jax.random.uniform(jax.random.fold_in(jax.random.fold_in(stream_key, 6), position), (shards_of,), jnp.float32, least / len(cuts), high / len(cuts))
        return jnp.repeat(jnp.exp(steps), dims[position] // shards_of).reshape((-1,) + (1,) * (len(dims) - position - 1))

    factor_of = one(*cuts[0])
    for cut in cuts[1:]:
        factor_of = factor_of * one(*cut)
    return factor_of


def profile(count, total, limit, lean):
    weights = [(1 << 20) // math.isqrt(standing ** lean) + 1 for standing in range(2, count + 1)]
    rest, given = total - limit - (count - 1), [1] * (count - 1)
    while rest > 0:
        free = [i for i in range(count - 1) if given[i] < limit]
        whole, budget = sum([weights[i] for i in free]), rest
        for i in free:
            addition = min(limit - given[i], max(1, budget * weights[i] // whole), rest)
            given[i] = given[i] + addition
            rest = rest - addition
    return np.array([limit] + given)


def uneven(own_key, count, total, bound, skew):
    if count == 2:
        one = jax.random.randint(own_key, (), max(1, total - bound), min(bound, total - 1) + 1)
        return jnp.stack([one, total - one])
    sizes = jnp.asarray(profile(count, total, bound, skew), jnp.int32)
    pairs = (count - 1) // 2
    source_of, taker = sizes[1:1 + 2 * pairs:2], sizes[2:2 + 2 * pairs:2]
    margin = jnp.minimum(source_of - 1, bound - taker)
    passed = jax.random.randint(jax.random.fold_in(own_key, 1), (pairs,), 0, 1 << 20) % (margin + 1)
    sizes = sizes.at[1:1 + 2 * pairs:2].set(source_of - passed).at[2:2 + 2 * pairs:2].set(taker + passed)
    return sizes[jax.random.permutation(jax.random.fold_in(own_key, 2), count)]


def normal_values(own_key, dims, width, most, cuts=(), held_as=jnp.bfloat16):
    values = jax.random.normal(own_key, dims, jnp.float32) * width
    if len(cuts) > 0:
        values = block_levels(own_key, dims, cuts, -0.22, 0.18) * values
    return jnp.clip(values, min=-most, max=most).astype(held_as)


def setup_inputs(seed: int = 0) -> dict:
    arg_keys = jax.random.split(jax.random.key(seed), 7)
    hidden_in = normal_values(arg_keys[0], (BATCH, SEQ, D), 1.0, 6.0, ((0, 2), (1, 128)))
    segment_ids = jax.vmap(lambda own: jnp.searchsorted(jnp.cumsum(uneven(own, DOCS, SEQ, DOC_MOST, 2)), jnp.arange(SEQ), side="right"))(jax.random.split(arg_keys[1], BATCH)).reshape((BATCH, SEQ)).astype(jnp.int32)
    pre_gain = jnp.clip(1.0 + 0.15 * jax.random.normal(arg_keys[2], (D,), jnp.float32), 0.25, 1.75)
    w_qkv = draw_w_qkv(jax.random.fold_in(arg_keys[6], 71), 0)
    w_out = normal_values(arg_keys[4], (ATT_W, D), ATT_W ** -0.5, 0.1875, ((0, 128),))
    post_gain = jnp.clip(1.0 + 0.15 * jax.random.normal(arg_keys[5], (D,), jnp.float32), 0.25, 1.75)
    return dict(hidden_in=hidden_in, segment_ids=segment_ids, pre_gain=pre_gain, w_qkv=w_qkv, w_out=w_out, post_gain=post_gain)


EPS = 1e-06
CAP = 50.0

def rms_scale(values, gain):
    return values * lax.rsqrt(lax.optimization_barrier(jnp.mean(values * values, axis=-1, keepdims=True)) + EPS) * gain

def barrier_round(values):
    return lax.optimization_barrier(values.astype(jnp.bfloat16)).astype(jnp.float32)

def rotary(values, positions):
    head_size = values.shape[-1]
    half_dim = head_size // 2
    inverse = 1.0 / 10000.0 ** (jnp.arange(half_dim, dtype=jnp.float32) * 2.0 / head_size)
    angles = positions.astype(jnp.float32)[:, None] * inverse[None, :]
    shape = (values.shape[0],) + (1,) * (values.ndim - 2) + (half_dim,)
    cosine = jnp.cos(angles).reshape(shape)
    sine = jnp.sin(angles).reshape(shape)
    first_half = values[..., :half_dim]
    second_half = values[..., half_dim:]
    return jnp.concatenate([first_half * cosine - second_half * sine, second_half * cosine + first_half * sine], axis=-1)

def one_sequence(inputs, segment_row, pre_gain, w_qkv, w_out, post_gain):
    seq_len = inputs.shape[0]
    groups = Q_HEADS // KV_HEADS
    widened = inputs.astype(jnp.float32)
    normed = rms_scale(widened, pre_gain).astype(jnp.bfloat16)
    projected = jnp.dot(normed, w_qkv, preferred_element_type=jnp.float32)
    positions = jnp.arange(seq_len, dtype=jnp.int32)
    queries = rotary(projected[:, :Q_HEADS * HEAD].reshape(seq_len, KV_HEADS, groups, HEAD), positions)
    key_rows = rotary(projected[:, Q_HEADS * HEAD:(Q_HEADS + KV_HEADS) * HEAD].reshape(seq_len, KV_HEADS, HEAD), positions)
    value_rows = projected[:, (Q_HEADS + KV_HEADS) * HEAD:].reshape(seq_len, KV_HEADS, HEAD)
    query_full = barrier_round(queries)
    key_full = barrier_round(key_rows)
    value_full = barrier_round(value_rows)
    doc_numbers = jnp.arange(DOCS, dtype=jnp.int32)
    matches = segment_row[:, None] == doc_numbers[None, :]
    first_pos = lax.optimization_barrier(jnp.min(jnp.where(matches, positions[:, None], seq_len), axis=0)).astype(jnp.int32)
    starts = lax.optimization_barrier(jnp.sum(jnp.where(matches, first_pos[None, :], 0), axis=1)).astype(jnp.int32)
    key_pad = jnp.concatenate([jnp.zeros((WINDOW, KV_HEADS, HEAD), jnp.float32), key_full], axis=0)
    value_pad = jnp.concatenate([jnp.zeros((WINDOW, KV_HEADS, HEAD), jnp.float32), value_full], axis=0)
    scale = 1.0 / math.sqrt(HEAD)

    def block(index):
        qstart = (index * TOK_DEV).astype(jnp.int32)
        query_block = lax.dynamic_slice_in_dim(query_full, qstart, TOK_DEV, 0)
        key_block = lax.dynamic_slice_in_dim(key_pad, qstart, WINDOW + TOK_DEV, 0)
        value_block = lax.dynamic_slice_in_dim(value_pad, qstart, WINDOW + TOK_DEV, 0)
        start_block = lax.dynamic_slice_in_dim(starts, qstart, TOK_DEV, 0)
        query_pos = qstart + jnp.arange(TOK_DEV, dtype=jnp.int32)
        key_pos = qstart - WINDOW + jnp.arange(WINDOW + TOK_DEV, dtype=jnp.int32)
        scores = jnp.einsum('qhgd,khd->qhgk', query_block, key_block) * scale
        capped = CAP * jnp.tanh(scores / CAP)
        allowed = (key_pos[None, :] <= query_pos[:, None]) & (query_pos[:, None] - key_pos[None, :] < WINDOW) & (key_pos[None, :] >= start_block[:, None])
        weights = jnp.where(allowed[:, None, None, :], jnp.exp(capped), 0.0)
        totals = lax.optimization_barrier(jnp.sum(weights, axis=-1))
        mixed = jnp.einsum('qhgk,khd->qhgd', barrier_round(weights), value_block)
        return (mixed / totals[..., None]).astype(jnp.bfloat16).reshape(TOK_DEV, Q_HEADS * HEAD)
    attended = lax.map(block, jnp.arange(seq_len // TOK_DEV, dtype=jnp.int32)).reshape(seq_len, Q_HEADS * HEAD)
    branch = jnp.dot(attended, w_out, preferred_element_type=jnp.float32)
    return (widened + rms_scale(branch, post_gain)).astype(jnp.bfloat16)

def reference(hidden_in, segment_ids, pre_gain, w_qkv, w_out, post_gain):
    results = []
    for row in range(BATCH):
        results.append(one_sequence(hidden_in[row], segment_ids[row], pre_gain, w_qkv, w_out, post_gain))
    return jnp.stack(results, axis=0)
```

```python
import jax
import jax.numpy as jnp
from jax import lax
from jax.experimental import pallas as pl
from jax.experimental.pallas import tpu as pltpu
from jax.sharding import PartitionSpec as P

MESH = pl.DeviceIdType.MESH
BF, F32, I32 = jnp.bfloat16, jnp.float32, jnp.int32

D = 2304
HEAD = 256
WINDOW = 4096
TOK = 256
CHIP = 512
SEQ_DEV = 128
LINES = 8
LROWS = 288
OROWS = 128
EPS = 1e-06
CAP = 50.0
LOG2E = 1.4426950408889634


def kernel(
    hid, seg, wqkv, wout, cos, sin, pre, post, out,
    H, N, W, WO, ZW, ZQ, ZO, FS, ACC, QQ, O, L, A, B, SEGW, QS, ATT, SB, BR,
    s_loc, s_z, r_z, s_s, r_s, s_y, r_y, s_x, r_x, s_a, r_a, s_b, r_b, s_m, r_m,
):
    seq = lax.axis_index("seq")
    bat = lax.axis_index("batch")
    core = lax.rem(seq, 2)
    other = 1 - core
    me = lax.rem(seq, 16)
    z = lax.div(me, 2)
    line = lax.div(seq, 16)
    y = lax.rem(line, 4)
    xl = lax.div(line, 4)

    def dev(s, b=bat):
        return {"seq": s, "batch": b}

    def at_line(xx, yy):
        return (xx * 4 + yy) * 16 + me

    yp, ym, y2 = lax.rem(y + 1, 4), lax.rem(y + 3, 4), lax.rem(y + 2, 4)
    up, down = dev(at_line(xl, yp)), dev(at_line(xl, ym))
    x0, x1 = dev(at_line(1 - xl, y)), dev(at_line(1 - xl, y), 1 - bat)
    nxt, prv = dev(lax.rem(seq + 2, SEQ_DEV)), dev(lax.rem(seq + 126, SEQ_DEV))
    nxt8, prv8 = dev(lax.rem(seq + 16, SEQ_DEV)), dev(lax.rem(seq + 112, SEQ_DEV))
    mate = dev(seq + 1 - 2 * core)

    def z_dev(d, c):
        return dev(line * 16 + lax.rem(z + d, 8) * 2 + c)

    def rc(src, dst, ss, rs, to):
        return pltpu.make_async_remote_copy(
            src_ref=src, dst_ref=dst, send_sem=ss, recv_sem=rs, device_id=to, device_id_type=MESH
        )

    def got(ref, rs):
        rc(ref, ref, s_m.at[0], rs, mate).wait_recv()

    sends = []

    def send(src, dst, ss, rs, to):
        copy = rc(src, dst, ss, rs, to)
        copy.start()
        sends.append(copy)

    barrier = pltpu.get_barrier_semaphore()

    def greet(to):
        pl.semaphore_signal(barrier, inc=1, device_id=to, device_id_type=MESH)

    @pl.loop(1, 8)
    def _(d):
        greet(z_dev(d, 0))
        greet(z_dev(d, 1))

    for to in (mate, up, down, x0, x1, nxt, prv, nxt8, prv8):
        greet(to)

    own = pl.ds(pl.multiple_of(core * TOK, TOK), TOK)
    local = [
        pltpu.make_async_copy(hid, H.at[own], s_loc.at[0]),
        pltpu.make_async_copy(
            wqkv.at[:, pl.ds(pl.multiple_of(1024 + 256 * core, 256), 256)],
            ZW.at[me, :, pl.ds(0, 256)],
            s_loc.at[1],
        ),
        pltpu.make_async_copy(
            wqkv.at[:, pl.ds(pl.multiple_of(1536 + 256 * core, 256), 256)],
            ZW.at[me, :, pl.ds(256, 256)],
            s_loc.at[2],
        ),
        pltpu.make_async_copy(
            wqkv.at[:, pl.ds(pl.multiple_of(512 * core, 512), 512)], ZQ.at[me], s_loc.at[3]
        ),
        pltpu.make_async_copy(
            wout.at[:, pl.ds(pl.multiple_of(1152 * core, 128), 1152)], ZO.at[me], s_loc.at[4]
        ),
        pltpu.make_async_copy(seg, SEGW.at[16 + me], s_loc.at[5]),
    ]
    for copy in local:
        copy.start()

    pl.semaphore_wait(barrier, 23)

    def z_copies(p, slot, c, to):
        if p == 0:
            src, dst = wqkv.at[:, pl.ds(pl.multiple_of(1024 + 256 * c, 256), 256)], ZW.at[me, :, pl.ds(0, 256)]
        elif p == 1:
            src, dst = wqkv.at[:, pl.ds(pl.multiple_of(1536 + 256 * c, 256), 256)], ZW.at[me, :, pl.ds(256, 256)]
        elif p == 2:
            src, dst = wqkv.at[:, pl.ds(pl.multiple_of(512 * c, 512), 512)], ZQ.at[me]
        else:
            src, dst = wout.at[:, pl.ds(pl.multiple_of(1152 * c, 128), 1152)], ZO.at[me]
        return rc(src, dst, s_z.at[p, slot], r_z.at[p, me], to)

    def z_send(*pieces):
        @pl.loop(1, 8)
        def _(d):
            for c in (0, 1):
                for p in pieces:
                    z_copies(p, 2 * d + c, c, z_dev(d, c)).start()

        for p in pieces:
            z_copies(p, 0, other, mate).start()

    def z_landing(p, i):
        if p == 0:
            return ZW.at[i, :, pl.ds(0, 256)]
        if p == 1:
            return ZW.at[i, :, pl.ds(256, 256)]
        return ZQ.at[i] if p == 2 else ZO.at[i]

    def z_got(*pieces):
        @pl.loop(1, 16)
        def _(i):
            j = lax.rem(me + i, 16)
            for p in pieces:
                got(z_landing(p, j), r_z.at[p, j])

    def seg_copy(slot, to):
        return rc(seg, SEGW.at[16 + me], s_s.at[slot], r_s.at[me], to)

    z_send(0, 1)
    send(hid, H.at[own], s_m.at[1], r_m.at[1], mate)

    @pl.loop(1, 8)
    def _(d):
        for c in (0, 1):
            seg_copy(2 * d + c, z_dev(d, c)).start()

    seg_copy(0, mate).start()
    z_send(2)
    z_send(3)

    def norm_rows(first):
        @pl.loop(0, TOK // 64)
        def _(i):
            rows = pl.ds(pl.multiple_of(first + i * 64, 64), 64)
            v = H[rows, :].astype(F32)
            v = v * lax.rsqrt(jnp.mean(v * v, axis=-1, keepdims=True) + EPS) * pre[...]
            v = v.astype(BF)
            N[0, rows, :] = v[:, : D // 2]
            N[1, rows, :] = v[:, D // 2 :]

    local[0].wait()
    norm_rows(core * TOK)
    theirs = pl.ds(pl.multiple_of(other * TOK, TOK), TOK)
    got(H.at[theirs], r_m.at[1])
    norm_rows(other * TOK)

    def part(s, yy, half, xx=xl):
        ln = xx * 4 + yy
        n = OROWS if s == 2 else LROWS
        first, size = (0, n) if half is None else (half * (n // 2), n // 2)
        rows = pl.ds(pl.multiple_of(ln * n + first, 16), size)
        if s == 2:
            return WO.at[core, rows, :]
        return W.at[rows, pl.ds(512 * s, 512)]

    def over(s, yy, half, k, to, sem_s, sem_r):
        ref = part(s, yy, half)
        send(ref, ref, sem_s.at[s, k], sem_r, to)

    def to_x(s, yy, half, k):
        over(s, yy, half, k, x1 if half else x0, s_x, r_x.at[s, yy * 2 + half])

    def stage1(s):
        over(s, y, None, 0, up, s_y, r_y.at[s, 0])
        over(s, y, None, 1, down, s_y, r_y.at[s, 1])
        to_x(s, y, 0, 0)
        to_x(s, y, 1, 1)

    def stage2(s):
        got(part(s, ym, None), r_y.at[s, 0])
        over(s, ym, 0, 2, up, s_y, r_y.at[s, 2])
        to_x(s, ym, 0, 2)
        to_x(s, ym, 1, 3)
        got(part(s, yp, None), r_y.at[s, 1])
        over(s, yp, 1, 3, down, s_y, r_y.at[s, 3])
        to_x(s, yp, 0, 4)
        to_x(s, yp, 1, 5)

    def stage3(s):
        got(part(s, y2, 0), r_y.at[s, 2])
        to_x(s, y2, 0, 6)
        got(part(s, y2, 1), r_y.at[s, 3])
        to_x(s, y2, 1, 7)

    def stage4(s):
        for yy in range(4):
            for half in (0, 1):
                got(part(s, yy, half, 1 - xl), r_x.at[s, yy * 2 + half])

    def repack(Z, col):
        for j in range(16):
            FS[pl.ds(18 * j, 18), :] = Z[j].astype(F32)
        W[pl.ds(pl.multiple_of(line * LROWS, 16), LROWS), pl.ds(col, 512)] = FS[...].astype(BF)

    z_got(0, 1)
    local[1].wait()
    local[2].wait()
    repack(ZW, 0)
    stage1(0)
    z_got(2)
    local[3].wait()
    repack(ZQ, 512)

    @pl.loop(1, 16)
    def _(i):
        j = lax.rem(me + i, 16)
        got(SEGW.at[16 + j], r_s.at[j])

    local[5].wait()
    send(SEGW.at[pl.ds(16, 16)], SEGW.at[pl.ds(0, 16)], s_m.at[2], r_m.at[2], nxt8)
    for half in (0, 1):
        row = SEGW[16 + 2 * z + half].astype(F32)
        QS[pl.ds(half * TOK, TOK), :] = jnp.broadcast_to(row, (TOK, TOK)).T

    stage2(0)
    stage3(0)
    stage1(1)

    def project(col, xx, add):
        @pl.loop(0, 2)
        def _(i):
            rows = pl.ds(pl.multiple_of(i * TOK, TOK), TOK)
            w = W[pl.ds(pl.multiple_of(xx * (D // 2), 16), D // 2), pl.ds(col, 512)]
            term = jnp.dot(N[xx, rows, :], w, preferred_element_type=F32)
            ACC[rows, :] = ACC[rows, :] + term if add else term

    def turned(rows, col):
        a, b = ACC[rows, pl.ds(col, 128)], ACC[rows, pl.ds(col + 128, 128)]
        c, s = cos[rows, :], sin[rows, :]
        return (a * c - b * s).astype(BF), (b * c + a * s).astype(BF)

    project(0, xl, False)
    stage4(0)
    project(0, 1 - xl, True)
    for half, buf in ((1, B), (0, A)):
        rows = pl.ds(half * TOK, TOK)
        low, high = turned(rows, 0)
        buf[0, 0, :, pl.ds(0, 128)] = low
        buf[0, 0, :, pl.ds(128, 128)] = high
        buf[0, 1] = ACC[rows, pl.ds(256, 256)].astype(BF)

    for kv in (0, 1):
        send(B.at[0, kv], B.at[8, kv], s_b.at[0, kv], r_b.at[8, kv], nxt8)
    for kv in (0, 1):
        send(A.at[0, kv], A.at[1, kv], s_a.at[0, kv], r_a.at[1, kv], nxt)
    for kv in (0, 1):
        send(A.at[0, kv], A.at[8, kv], s_a.at[8, kv], r_a.at[8, kv], nxt8)

    got(SEGW.at[pl.ds(0, 16)], r_m.at[2])

    def pass_a(j, kv):
        return rc(A.at[j, kv], A.at[j + 1, kv], s_a.at[j, kv], r_a.at[j + 1, kv], nxt)

    def pass_b(t, kv):
        return rc(B.at[t, kv], B.at[t - 1, kv], s_b.at[t, kv], r_b.at[t - 1, kv], prv)

    def relay(j):
        t = 9 - j
        for kv in (0, 1):
            got(A.at[j, kv], r_a.at[j, kv])

            @pl.when(j <= 6)
            def _():
                pass_a(j, kv).start()

            got(B.at[t, kv], r_b.at[t, kv])

            @pl.when(j <= 7)
            def _():
                pass_b(t, kv).start()

    stage2(1)
    stage3(1)
    relay(1)
    project(512, xl, False)
    stage4(1)
    project(512, 1 - xl, True)
    for h in (0, 1):
        for half in (0, 1):
            rows = pl.ds(half * TOK, TOK)
            low, high = turned(rows, 256 * h)
            dst = pl.ds(h * CHIP + half * TOK, TOK)
            QQ[dst, pl.ds(0, 128)] = low
            QQ[dst, pl.ds(128, 128)] = high

    O[...] = jnp.zeros_like(O)
    L[...] = jnp.zeros_like(L)

    def attend(buf, t, half):
        index = 16 + 2 * z + half - 2 * t
        shut = jnp.logical_and(index < 16, line == 0)
        docs = jnp.where(shut, -1.0, SEGW[index].astype(F32))
        first = half * TOK - CHIP * t

        @pl.loop(0, 4)
        def _(r):
            rows = pl.ds(pl.multiple_of(r * TOK, TOK), TOK)
            tok = pl.multiple_of(lax.rem(r, 2) * TOK, TOK)
            s = lax.dot_general(
                QQ[rows, :], buf[t, 0], (((1,), (1,)), ((), ())), preferred_element_type=F32
            )
            w = jnp.exp2(jnp.tanh(s * (1.0 / (16.0 * CAP))) * (CAP * LOG2E))
            behind = (
                lax.broadcasted_iota(I32, (TOK, TOK), 0)
                - lax.broadcasted_iota(I32, (TOK, TOK), 1)
                + (tok - first)
            )
            allowed = (behind >= 0) & (behind < WINDOW) & (QS[pl.ds(tok, TOK), :] == docs)
            w = jnp.where(allowed, w, 0.0)
            L[rows, :] += w[:, :128] + w[:, 128:]
            O[rows, :] += jnp.dot(w.astype(BF), buf[t, 1], preferred_element_type=F32)

    z_got(3)
    local[4].wait()
    for j in range(0, 16, 2):
        pair = jnp.concatenate([ZO[j].astype(F32), ZO[j + 1].astype(F32)], axis=0)
        WO[core, pl.ds(pl.multiple_of(line * OROWS + 8 * j, 16), 16), :] = pair.astype(BF)
    stage1(2)

    attend(B, 0, 1)
    attend(A, 0, 0)
    attend(A, 1, 0)
    attend(B, 8, 1)

    def step(j):
        relay(j)
        attend(A, j, 0)
        attend(B, 9 - j, 1)

    step(2)
    stage2(2)
    step(3)
    stage3(2)
    step(4)
    step(5)
    stage4(2)
    send(WO.at[core], WO.at[core], s_m.at[3], r_m.at[3], mate)
    pl.loop(6, 9)(step)

    for g in (0, 1):
        @pl.when(core == g)
        def _():
            for h in (0, 1):
                for half in (0, 1):
                    rows = pl.ds(h * CHIP + half * TOK, TOK)
                    att = O[rows, :] / jnp.sum(L[rows, :], axis=-1, keepdims=True)
                    if half == g:
                        ATT[g, :, pl.ds(h * HEAD, HEAD)] = att.astype(BF)
                    else:
                        SB[:, pl.ds(h * HEAD, HEAD)] = att.astype(BF)

    send(SB, ATT.at[core], s_m.at[4], r_m.at[4], mate)
    got(WO.at[other], r_m.at[3])
    got(ATT.at[other], r_m.at[4])

    for c in (0, 1):
        cols = pl.ds(c * (D // 2), D // 2)
        BR[:, cols] = jnp.dot(ATT[0], WO[c, pl.ds(0, 512), :], preferred_element_type=F32) + jnp.dot(
            ATT[1], WO[c, pl.ds(512, 512), :], preferred_element_type=F32
        )

    @pl.loop(0, TOK // 32)
    def _(i):
        rows = pl.ds(pl.multiple_of(i * 32, 32), 32)
        v = BR[rows, :]
        v = v * lax.rsqrt(jnp.mean(v * v, axis=-1, keepdims=True) + EPS) * post[...]
        x = H[pl.ds(pl.multiple_of(core * TOK + i * 32, 32), 32), :].astype(F32)
        out[rows, :] = (x + v).astype(BF)

    for copy in sends:
        copy.wait_send()

    @pl.loop(1, 8)
    def _(j):
        for kv in (0, 1):
            @pl.when(j <= 6)
            def _():
                pass_a(j, kv).wait_send()

            pass_b(9 - j, kv).wait_send()

    @pl.loop(1, 8)
    def _(d):
        for c in (0, 1):
            seg_copy(2 * d + c, z_dev(d, c)).wait_send()
            for p in range(4):
                z_copies(p, 2 * d + c, c, z_dev(d, c)).wait_send()

    seg_copy(0, mate).wait_send()
    for p in range(4):
        z_copies(p, 0, other, mate).wait_send()


def per_device(hidden_in, segment_ids, pre_gain, w_qkv, w_out, post_gain):
    chip = lax.axis_index("seq") // 2
    positions = chip * CHIP + jnp.arange(CHIP, dtype=I32)
    inverse = 1.0 / 10000.0 ** (jnp.arange(HEAD // 2, dtype=F32) * 2.0 / HEAD)
    angles = positions.astype(F32)[:, None] * inverse[None, :]
    hbm = pl.BlockSpec(memory_space=pltpu.HBM)
    vmem = pl.BlockSpec(memory_space=pltpu.VMEM)
    dma = pltpu.SemaphoreType.DMA
    result = pl.pallas_call(
        kernel,
        out_shape=jax.ShapeDtypeStruct((TOK, D), BF),
        in_specs=[hbm] * 4 + [vmem] * 4,
        out_specs=vmem,
        scratch_shapes=[
            pltpu.VMEM((CHIP, D), BF),
            pltpu.VMEM((2, CHIP, D // 2), BF),
            pltpu.VMEM((D, 1024), BF),
            pltpu.VMEM((2, 1024, D // 2), BF),
            pltpu.VMEM((16, 18, 512), BF),
            pltpu.VMEM((16, 18, 512), BF),
            pltpu.VMEM((16, 8, D // 2), BF),
            pltpu.VMEM((LROWS, 512), F32),
            pltpu.VMEM((CHIP, 512), F32),
            pltpu.VMEM((2 * CHIP, HEAD), BF),
            pltpu.VMEM((2 * CHIP, HEAD), F32),
            pltpu.VMEM((2 * CHIP, 128), F32),
            pltpu.VMEM((9, 2, TOK, HEAD), BF),
            pltpu.VMEM((9, 2, TOK, HEAD), BF),
            pltpu.VMEM((32, 1, TOK), I32),
            pltpu.VMEM((CHIP, TOK), F32),
            pltpu.VMEM((2, TOK, 512), BF),
            pltpu.VMEM((TOK, 512), BF),
            pltpu.VMEM((TOK, D), F32),
            dma((6,)),
            dma((4, 16)), dma((4, 16)),
            dma((16,)), dma((16,)),
            dma((3, 4)), dma((3, 4)),
            dma((3, 8)), dma((3, 8)),
            dma((9, 2)), dma((9, 2)),
            dma((9, 2)), dma((9, 2)),
            dma((5,)), dma((5,)),
        ],
        compiler_params=pltpu.CompilerParams(
            collective_id=0, has_side_effects=True, vmem_limit_bytes=60 * 1024 * 1024
        ),
    )(
        hidden_in[0],
        segment_ids,
        w_qkv,
        w_out,
        jnp.cos(angles),
        jnp.sin(angles),
        pre_gain.reshape(1, D),
        post_gain.reshape(1, D),
    )
    return result[None]


def solution(mesh):
    placed = (P("batch", "seq", None), P("batch", "seq"), P(), P("seq", None), P("seq", None), P())
    return jax.shard_map(
        per_device, mesh=mesh, in_specs=placed, out_specs=P("batch", "seq", None), check_vma=False
    )
```

```python
import jax
import jax.numpy as jnp
from jax import lax
from jax.experimental import pallas as pl
from jax.experimental.pallas import tpu as pltpu
from jax.sharding import PartitionSpec as P

MESH = pl.DeviceIdType.MESH
BF, F32, I32 = jnp.bfloat16, jnp.float32, jnp.int32

D = 2304
HEAD = 256
WINDOW = 4096
TOK = 256
CHIP = 512
SEQ_DEV = 128
LINES = 8
LROWS = 288
OROWS = 128
LAG = 3
EPS = 1e-06
CAP = 50.0
LOG2E = 1.4426950408889634


def kernel(
    hid, seg, wqkv, wout, inverse, pre18, post18, out,
    cos, sin, pre, post, H, N, W, WO, ZW, ZQ, ZO, FS, ACC, QQ, O, L, A, B, RA, RB, SEGW, QS, ATT, SB, BR,
    s_loc, s_z, r_z, s_y, r_y, s_x, r_x, s_a, r_a, s_b, r_b, s_d, r_d, s_m, r_m,
):
    seq = lax.axis_index("seq")
    bat = lax.axis_index("batch")
    core = lax.rem(seq, 2)
    other = 1 - core
    me = lax.rem(seq, 16)
    z = lax.div(me, 2)
    line = lax.div(seq, 16)
    y = lax.rem(line, 4)
    xl = lax.div(line, 4)

    def dev(s, b=bat):
        return {"seq": s, "batch": b}

    def at_line(xx, yy):
        return (xx * 4 + yy) * 16 + me

    yp, ym, y2 = lax.rem(y + 1, 4), lax.rem(y + 3, 4), lax.rem(y + 2, 4)
    up, down = dev(at_line(xl, yp)), dev(at_line(xl, ym))
    x0, x1 = dev(at_line(1 - xl, y)), dev(at_line(1 - xl, y), 1 - bat)
    nxt, prv = dev(lax.rem(seq + 2, SEQ_DEV)), dev(lax.rem(seq + 126, SEQ_DEV))
    nxt8, prv8 = dev(lax.rem(seq + 16, SEQ_DEV)), dev(lax.rem(seq + 112, SEQ_DEV))
    mate = dev(seq + 1 - 2 * core)
    z0, z7 = dev(line * 16 + core), dev(line * 16 + 14 + core)

    def z_dev(d, c):
        return dev(line * 16 + lax.rem(z + d, 8) * 2 + c)

    def rc(src, dst, ss, rs, to):
        return pltpu.make_async_remote_copy(
            src_ref=src, dst_ref=dst, send_sem=ss, recv_sem=rs, device_id=to, device_id_type=MESH
        )

    def got(ref, rs):
        rc(ref, ref, s_m.at[0], rs, mate).wait_recv()

    def gone(ref, ss):
        rc(ref, ref, ss, r_m.at[0], mate).wait_send()

    sends = []

    def send(src, dst, ss, rs, to):
        copy = rc(src, dst, ss, rs, to)
        copy.start()
        sends.append(copy)

    barrier = pltpu.get_barrier_semaphore()

    def greet(to):
        pl.semaphore_signal(barrier, inc=1, device_id=to, device_id_type=MESH)

    @pl.loop(1, 8)
    def _(d):
        greet(z_dev(d, 0))
        greet(z_dev(d, 1))

    for to in (mate, up, down, x0, x1, nxt, prv, nxt8, prv8):
        greet(to)

    own = pl.ds(pl.multiple_of(core * TOK, TOK), TOK)
    local = [
        pltpu.make_async_copy(hid, H.at[own], s_loc.at[0]),
        pltpu.make_async_copy(
            wqkv.at[:, pl.ds(pl.multiple_of(1024 + 256 * core, 256), 256)],
            ZW.at[me, :, pl.ds(0, 256)],
            s_loc.at[1],
        ),
        pltpu.make_async_copy(
            wqkv.at[:, pl.ds(pl.multiple_of(1536 + 256 * core, 256), 256)],
            ZW.at[me, :, pl.ds(256, 256)],
            s_loc.at[2],
        ),
        pltpu.make_async_copy(
            wqkv.at[:, pl.ds(pl.multiple_of(512 * core, 512), 512)], ZQ.at[me], s_loc.at[3]
        ),
        pltpu.make_async_copy(
            wout.at[:, pl.ds(pl.multiple_of(1152 * core, 128), 1152)], ZO.at[me], s_loc.at[4]
        ),
        pltpu.make_async_copy(seg, SEGW.at[16 + me], s_loc.at[5]),
    ]
    for copy in local:
        copy.start()

    pl.semaphore_wait(barrier, 23)

    def z_copies(p, c, to):
        if p == 0:
            src, dst = wqkv.at[:, pl.ds(pl.multiple_of(1024 + 256 * c, 256), 256)], ZW.at[me, :, pl.ds(0, 256)]
        elif p == 1:
            src, dst = wqkv.at[:, pl.ds(pl.multiple_of(1536 + 256 * c, 256), 256)], ZW.at[me, :, pl.ds(256, 256)]
        elif p == 2:
            src, dst = wqkv.at[:, pl.ds(pl.multiple_of(512 * c, 512), 512)], ZQ.at[me]
        else:
            src, dst = wout.at[:, pl.ds(pl.multiple_of(1152 * c, 128), 1152)], ZO.at[me]
        return rc(src, dst, s_z.at[p], r_z.at[p], to)

    def z_send(*pieces):
        @pl.loop(1, 8)
        def _(d):
            for c in (0, 1):
                for p in pieces:
                    z_copies(p, c, z_dev(d, c)).start()

        for p in pieces:
            z_copies(p, other, mate).start()

    def z_others(p):
        if p == 0:
            return ZW.at[pl.ds(0, 15), :, pl.ds(0, 256)]
        if p == 1:
            return ZW.at[pl.ds(0, 15), :, pl.ds(256, 256)]
        return ZQ.at[pl.ds(0, 15)] if p == 2 else ZO.at[pl.ds(0, 15)]

    def z_got(*pieces):
        for p in pieces:
            got(z_others(p), r_z.at[p])

    def seg_copy(to):
        return rc(seg, SEGW.at[16 + me], s_m.at[5], r_m.at[5], to)

    z_send(0, 1)
    send(hid, H.at[own], s_m.at[1], r_m.at[1], mate)

    @pl.loop(1, 8)
    def _(d):
        for c in (0, 1):
            seg_copy(z_dev(d, c)).start()

    seg_copy(mate).start()

    def norm_rows(first):
        @pl.loop(0, TOK // 64)
        def _(i):
            rows = pl.ds(pl.multiple_of(first + i * 64, 64), 64)
            v = H[rows, :].astype(F32)
            v = v * lax.rsqrt(jnp.mean(v * v, axis=-1, keepdims=True) + EPS) * pre[...]
            v = v.astype(BF)
            N[0, rows, :] = v[:, : D // 2]
            N[1, rows, :] = v[:, D // 2 :]

    for i in range(D // 128):
        pre[:, pl.ds(128 * i, 128)] = pre18[pl.ds(i, 1), :]
        post[:, pl.ds(128 * i, 128)] = post18[pl.ds(i, 1), :]
    local[0].wait()
    norm_rows(core * TOK)
    theirs = pl.ds(pl.multiple_of(other * TOK, TOK), TOK)
    got(H.at[theirs], r_m.at[1])
    norm_rows(other * TOK)

    @pl.loop(0, CHIP // 64)
    def _(i):
        rows = pl.ds(pl.multiple_of(i * 64, 64), 64)
        places = lax.div(seq, 2) * CHIP + i * 64 + lax.broadcasted_iota(I32, (64, HEAD // 2), 0)
        angles = places.astype(F32) * inverse[...]
        cos[rows, :] = jnp.cos(angles)
        sin[rows, :] = jnp.sin(angles)

    def part(s, yy, half, xx=xl):
        ln = xx * 4 + yy
        n = OROWS if s == 2 else LROWS
        first, size = (0, n) if half is None else (half * (n // 2), n // 2)
        rows = pl.ds(pl.multiple_of(ln * n + first, 16), size)
        if s == 2:
            return WO.at[core, rows, :]
        return W.at[rows, pl.ds(512 * s, 512)]

    def to_y(s, yy, half, to, k):
        ref = part(s, yy, half)
        rc(ref, ref, s_y.at[s], r_y.at[s, k], to).start()

    def to_x(s, yy, half):
        ref = part(s, yy, half)
        rc(ref, ref, s_x.at[s], r_x.at[s], x1 if half else x0).start()

    def stage1_up(s):
        to_y(s, y, 0, up, 0)
        to_y(s, y, 1, up, 1)

    def stage1(s):
        to_y(s, y, 1, down, 3)
        to_y(s, y, 0, down, 2)
        to_x(s, y, 0)
        to_x(s, y, 1)

    def from_below(s, half):
        got(part(s, ym, half), r_y.at[s, half])
        if s == 0 and half == 0:
            to_y(s, ym, 0, up, 4)
        to_x(s, ym, half)

    def from_above(s, half):
        got(part(s, yp, half), r_y.at[s, 2 + half])
        if s > 0 or half == 1:
            to_y(s, yp, half, down, 4 + half)
        to_x(s, yp, half)

    def stage2_up(s):
        from_below(s, 0)
        from_below(s, 1)

    def stage2(s):
        from_above(s, 1)
        from_above(s, 0)

    def from_second(s, half):
        got(part(s, y2, half), r_y.at[s, 4 + half])
        to_x(s, y2, half)

    def stage3(s):
        from_second(s, 0)
        from_second(s, 1)

    def stage4(s):
        n = 4 * (OROWS if s == 2 else LROWS)
        first = pl.multiple_of((1 - xl) * n, 16)
        if s == 2:
            got(WO.at[core, pl.ds(first, n), :], r_x.at[s])
        else:
            got(W.at[pl.ds(first, n), pl.ds(512 * s, 512)], r_x.at[s])

    def streams_gone(s):
        n = OROWS if s == 2 else LROWS
        for rows, sem in ((3 * n, s_y.at[s]), (4 * n, s_x.at[s])):
            if s == 2:
                gone(WO.at[core, pl.ds(0, rows), :], sem)
            else:
                gone(W.at[pl.ds(0, rows), pl.ds(512 * s, 512)], sem)

    def repack(Z, col):
        for j in range(16):
            FS[pl.ds(18 * j, 18), :] = Z[j].astype(F32)
        W[pl.ds(pl.multiple_of(line * LROWS, 16), LROWS), pl.ds(col, 512)] = FS[...].astype(BF)

    z_got(0, 1)
    local[1].wait()
    local[2].wait()
    repack(ZW, 0)
    stage1_up(0)
    stage1(0)
    z_send(2)
    from_below(0, 0)
    from_above(0, 1)
    from_below(0, 1)
    from_above(0, 0)
    z_send(3)
    stage3(0)
    z_got(2)
    local[3].wait()
    repack(ZQ, 512)
    stage1_up(1)
    stage1(1)

    def project(col, xx, add):
        @pl.loop(0, 2)
        def _(i):
            rows = pl.ds(pl.multiple_of(i * TOK, TOK), TOK)
            w = W[pl.ds(pl.multiple_of(xx * (D // 2), 16), D // 2), pl.ds(col, 512)]
            term = jnp.dot(N[xx, rows, :], w, preferred_element_type=F32)
            ACC[rows, :] = ACC[rows, :] + term if add else term

    def turned(rows, col):
        a, b = ACC[rows, pl.ds(col, 128)], ACC[rows, pl.ds(col + 128, 128)]
        c, s = cos[rows, :], sin[rows, :]
        return (a * c - b * s).astype(BF), (b * c + a * s).astype(BF)

    project(0, xl, False)

    got(SEGW.at[pl.ds(16, 15)], r_m.at[5])
    local[5].wait()
    send(SEGW.at[pl.ds(16, 16)], SEGW.at[pl.ds(0, 16)], s_m.at[2], r_m.at[2], nxt8)
    for half in (0, 1):
        row = SEGW[16 + 2 * z + half].astype(F32)
        QS[pl.ds(half * TOK, TOK), :] = jnp.broadcast_to(row, (TOK, TOK)).T

    stage4(0)
    project(0, 1 - xl, True)
    for half, buf in ((1, B), (0, A)):
        rows = pl.ds(half * TOK, TOK)
        low, high = turned(rows, 0)
        buf[0, 0, :, pl.ds(0, 128)] = low
        buf[0, 0, :, pl.ds(128, 128)] = high
        buf[0, 1] = ACC[rows, pl.ds(256, 256)].astype(BF)

    def piece(buf, t, c):
        return buf.at[t, c // 2, pl.ds(c % 2 * 128, 128), :]

    def stop(buf, k, c):
        return buf.at[k, pl.ds(c % 2 * 128, 128), :]

    def pass_on(buf, t, u, c, ss, rs, to):
        rc(piece(buf, t, c), piece(buf, u, c), ss, rs.at[u, c], to).start()

    def pass_a(j, c):
        @pl.when(z != 7)
        def _():
            pass_on(A, j, j + 1, c, s_a.at[0], r_a, nxt)

        @pl.when(z == 7)
        def _():
            to = nxt8 if c < 2 else z0
            rc(piece(A, j, c), stop(RA, j, c), s_a.at[0], r_d.at[0, j, c % 2], to).start()

    def pass_b(j, c):
        t = 9 - j

        @pl.when(z != 0)
        def _():
            pass_on(B, t, t - 1, c, s_b.at[0], r_b, prv)

        @pl.when(z == 0)
        def _():
            to = z7 if c < 2 else prv8
            rc(piece(B, t, c), stop(RB, j - 1, c), s_b.at[0], r_d.at[1, j - 1, c % 2], to).start()

    def take_a(e):
        j, c = divmod(e, 4)
        if 1 <= j <= 8:
            got(piece(A, j, c), r_a.at[j, c])
        if 1 <= j <= 6:
            pass_a(j, c)

    def take_b(e):
        j, c = divmod(e, 4)
        if 1 <= j <= 8:
            got(piece(B, 9 - j, c), r_b.at[9 - j, c])
        if 1 <= j <= 7:
            pass_b(j, c)

    def help_on(e, here):
        j, c = divmod(e, 4)
        if here != (7 if c < 2 else 0):
            return
        if 0 <= j <= 6:
            ref = stop(RA, j, c)
            got(ref, r_d.at[0, j, c % 2])
            to = z0 if c < 2 else nxt8
            rc(ref, piece(A, j + 1, c), s_d.at[0], r_a.at[j + 1, c], to).start()
        if 1 <= j <= 7:
            ref = stop(RB, j - 1, c)
            got(ref, r_d.at[1, j - 1, c % 2])
            to = prv8 if c < 2 else z7
            rc(ref, piece(B, 8 - j, c), s_d.at[0], r_b.at[8 - j, c], to).start()

    def relay(e):
        @pl.when(z == 0)
        def _():
            take_b(e)
            help_on(e - LAG, 0)
            take_a(e - LAG)

        @pl.when(z == 7)
        def _():
            take_a(e)
            help_on(e - LAG, 7)
            take_b(e - LAG)

        @pl.when((z > 0) & (z < 4))
        def _():
            take_b(e)
            take_a(e)

        @pl.when((z > 3) & (z < 7))
        def _():
            take_a(e)
            take_b(e)

    for c in range(4):
        pass_on(B, 0, 8, c, s_b.at[1], r_b, nxt8)
        pass_a(0, c)

    def attend(j, part):
        blocks = ((A, 0, 0), (B, 0, 1)) if j == 0 else ((A, j, 0), (B, 9 - j, 1))
        docs, firsts = [], []
        for _, t, half in blocks:
            index = 16 + 2 * z + half - 2 * t
            shut = jnp.logical_and(index < 16, line == 0)
            docs.append(jnp.where(shut, -1.0, SEGW[index].astype(F32)))
            firsts.append(half * TOK - CHIP * t)

        @pl.loop(2 * part, 2 * part + 2, unroll=2)
        def _(r):
            rows = pl.ds(pl.multiple_of(r * TOK, TOK), TOK)
            tok = pl.multiple_of(lax.rem(r, 2) * TOK, TOK)
            queries, whose = QQ[rows, :], QS[pl.ds(tok, TOK), :]
            sums, mixed = None, None
            for (buf, t, _), doc, first in zip(blocks, docs, firsts):
                s = lax.dot_general(
                    queries, buf[t, 0], (((1,), (1,)), ((), ())), preferred_element_type=F32
                )
                w = jnp.exp2(jnp.tanh(s * (1.0 / (16.0 * CAP))) * (CAP * LOG2E))
                allowed = whose == doc
                if t in (0, 8):
                    behind = (
                        lax.broadcasted_iota(I32, (TOK, TOK), 0)
                        - lax.broadcasted_iota(I32, (TOK, TOK), 1)
                        + (tok - first)
                    )
                    allowed &= (behind >= 0) & (behind < WINDOW)
                w = jnp.where(allowed, w, 0.0)
                part_sum = w[:, :128] + w[:, 128:]
                term = jnp.dot(w.astype(BF), buf[t, 1], preferred_element_type=F32)
                sums = part_sum if sums is None else sums + part_sum
                mixed = term if mixed is None else mixed + term
            if j == 0:
                L[rows, :] = sums
                O[rows, :] = mixed
            else:
                L[rows, :] += sums
                O[rows, :] += mixed

    def relays(first, last):
        for e in range(first, last):
            relay(e)
            for action in extra.get(e, ()):
                action()

    eighth = [lambda c=c: pass_on(A, 0, 8, c, s_a.at[1], r_a, nxt8) for c in range(4)]
    extra = {
        11: [lambda: to_y(2, y, 0, up, 0)],
        12: [lambda: to_y(2, y, 1, down, 3)],
        14: [lambda: to_y(2, y, 1, up, 1)],
        16: [lambda: to_y(2, y, 0, down, 2), lambda: to_x(2, y, 0), lambda: to_x(2, y, 1)],
        17: [eighth[0]],
        18: [lambda: from_above(2, 1)],
        19: [eighth[1]],
        20: [lambda: from_below(2, 0)],
        21: [eighth[2]],
        22: [lambda: from_above(2, 0)],
        23: [eighth[3]],
        24: [lambda: from_below(2, 1)],
        27: [lambda: from_second(2, 1)],
        29: [lambda: from_second(2, 0)],
        33: [
            lambda: stage4(2),
            lambda: send(WO.at[core], WO.at[core], s_m.at[3], r_m.at[3], mate),
        ],
    }

    relays(LAG, 8)
    stage2(1)

    z_got(3)
    local[4].wait()
    for j in range(0, 16, 2):
        pair = jnp.concatenate([ZO[j].astype(F32), ZO[j + 1].astype(F32)], axis=0)
        WO[core, pl.ds(pl.multiple_of(line * OROWS + 8 * j, 16), 16), :] = pair.astype(BF)

    gone(SEGW.at[pl.ds(0, 15)], s_m.at[5])
    for p in range(4):
        gone(z_others(p), s_z.at[p])

    relays(8, 12)
    stage2_up(1)
    stage3(1)
    relays(12, 14)
    project(512, xl, False)
    relays(14, 16)
    stage4(1)
    project(512, 1 - xl, True)
    for h in (0, 1):
        for half in (0, 1):
            rows = pl.ds(half * TOK, TOK)
            low, high = turned(rows, 256 * h)
            dst = pl.ds(h * CHIP + half * TOK, TOK)
            QQ[dst, pl.ds(0, 128)] = low
            QQ[dst, pl.ds(128, 128)] = high
    got(SEGW.at[pl.ds(0, 16)], r_m.at[2])

    todo = [(j, p) for j in range(9) for p in (0, 1)]
    for e in range(16, 36 + LAG):
        relays(e, e + 1)
        if todo and 4 * todo[0][0] + 3 + LAG <= e:
            attend(*todo.pop(0))
    for j, p in todo:
        attend(j, p)

    def attended(half, put):
        for h in (0, 1):
            rows = pl.ds(pl.multiple_of(h * CHIP + half * TOK, TOK), TOK)
            share = 1.0 / jnp.sum(L[rows, :], axis=-1, keepdims=True)
            put(h, (O[rows, :] * share).astype(BF))

    def put_other(h, value):
        SB[:, pl.ds(h * HEAD, HEAD)] = value

    def put_own(h, value):
        ATT[core, :, pl.ds(h * HEAD, HEAD)] = value

    attended(other, put_other)
    send(SB, ATT.at[core], s_m.at[4], r_m.at[4], mate)
    attended(core, put_own)
    got(WO.at[other], r_m.at[3])

    def branch(g, add):
        for c in (0, 1):
            cols = pl.ds(c * (D // 2), D // 2)
            weights = WO[c, pl.ds(pl.multiple_of(g * 512, 512), 512), :]
            term = jnp.dot(ATT[g], weights, preferred_element_type=F32)
            BR[:, cols] = BR[:, cols] + term if add else term

    branch(core, False)
    got(ATT.at[other], r_m.at[4])
    branch(other, True)

    @pl.loop(0, TOK // 32)
    def _(i):
        rows = pl.ds(pl.multiple_of(i * 32, 32), 32)
        v = BR[rows, :]
        v = v * lax.rsqrt(jnp.mean(v * v, axis=-1, keepdims=True) + EPS) * post[...]
        x = H[pl.ds(pl.multiple_of(core * TOK + i * 32, 32), 32), :].astype(F32)
        out[rows, :] = (x + v).astype(BF)

    for copy in sends:
        copy.wait_send()
    for buf, sem in ((A, s_a), (B, s_b)):
        gone(buf.at[pl.ds(0, 7)], sem.at[0])
        gone(buf.at[0], sem.at[1])
    @pl.when(lax.rem(z, 7) == 0)
    def _():
        gone(A.at[pl.ds(0, 7)], s_d.at[0])

    for stream in range(3):
        streams_gone(stream)


def per_device(hidden_in, segment_ids, pre_gain, w_qkv, w_out, post_gain):
    inverse = 1.0 / 10000.0 ** (jnp.arange(HEAD // 2, dtype=F32) * 2.0 / HEAD)
    hbm = pl.BlockSpec(memory_space=pltpu.HBM)
    vmem = pl.BlockSpec(memory_space=pltpu.VMEM)
    dma = pltpu.SemaphoreType.DMA
    result = pl.pallas_call(
        kernel,
        out_shape=pltpu.VMEM((TOK, D), BF),
        in_specs=[hbm] * 4 + [vmem] * 3,
        out_specs=vmem,
        scratch_shapes=[
            pltpu.VMEM((CHIP, HEAD // 2), F32),
            pltpu.VMEM((CHIP, HEAD // 2), F32),
            pltpu.VMEM((1, D), F32),
            pltpu.VMEM((1, D), F32),
            pltpu.VMEM((CHIP, D), BF),
            pltpu.VMEM((2, CHIP, D // 2), BF),
            pltpu.VMEM((D, 1024), BF),
            pltpu.VMEM((2, 1024, D // 2), BF),
            pltpu.VMEM((16, 18, 512), BF),
            pltpu.VMEM((16, 18, 512), BF),
            pltpu.VMEM((16, 8, D // 2), BF),
            pltpu.VMEM((LROWS, 512), F32),
            pltpu.VMEM((CHIP, 512), F32),
            pltpu.VMEM((2 * CHIP, HEAD), BF),
            pltpu.VMEM((2 * CHIP, HEAD), F32),
            pltpu.VMEM((2 * CHIP, 128), F32),
            pltpu.VMEM((9, 2, TOK, HEAD), BF),
            pltpu.VMEM((9, 2, TOK, HEAD), BF),
            pltpu.VMEM((7, TOK, HEAD), BF),
            pltpu.VMEM((7, TOK, HEAD), BF),
            pltpu.VMEM((32, 1, TOK), I32),
            pltpu.VMEM((CHIP, TOK), F32),
            pltpu.VMEM((2, TOK, 512), BF),
            pltpu.VMEM((TOK, 512), BF),
            pltpu.VMEM((TOK, D), F32),
            dma((6,)),
            dma((4,)), dma((4,)),
            dma((3,)), dma((3, 6)),
            dma((3,)), dma((3,)),
            dma((2,)), dma((9, 4)),
            dma((2,)), dma((9, 4)),
            dma((1,)), dma((2, 7, 2)),
            dma((6,)), dma((6,)),
        ],
        compiler_params=pltpu.CompilerParams(
            collective_id=0, has_side_effects=True, vmem_limit_bytes=60 * 1024 * 1024
        ),
    )(
        hidden_in[0],
        segment_ids,
        w_qkv,
        w_out,
        inverse.reshape(1, HEAD // 2),
        pre_gain.reshape(D // 128, 128),
        post_gain.reshape(D // 128, 128),
    )
    return result[None]


def solution(mesh):
    placed = (P("batch", "seq", None), P("batch", "seq"), P(), P("seq", None), P("seq", None), P())
    return jax.shard_map(
        per_device, mesh=mesh, in_specs=placed, out_specs=P("batch", "seq", None), check_vma=False
    )
```

```python
import jax
import jax.numpy as jnp
import numpy as np
from jax import lax
from jax.experimental import pallas as pl
from jax.experimental.pallas import tpu as pltpu
from jax.sharding import PartitionSpec as P

MESH = pl.DeviceIdType.MESH
BF, F32, I32 = jnp.bfloat16, jnp.float32, jnp.int32

D = 2304
HEAD = 256
WINDOW = 4096
TOK = 256
CHIP = 512
SEQ_DEV = 128
LINES = 8
LROWS = 288
OROWS = 128
LAGS = (2, 4, 3)
LAG = max(LAGS)
Q_AT = 19
EPS = 1e-06
CAP = 50.0
LOG2E = 1.4426950408889634


def kernel(
    hid, seg, wqkv, wout, inverse, pre18, post18, out,
    cos, sin, pre, post, H, N, W, WO, ZW, ZQ, ZO, FS, ACC, QQ, O, L, A, B, RA, RB, SEGW, QS, ATT, SB, BR,
    s_loc, s_z, r_z, s_f, r_f, s_y, r_y, s_x, r_x, s_a, r_a, s_b, r_b, s_d, r_d, s_m, r_m,
):
    seq = lax.axis_index("seq")
    bat = lax.axis_index("batch")
    core = lax.rem(seq, 2)
    other = 1 - core
    me = lax.rem(seq, 16)
    z = lax.div(me, 2)
    line = lax.div(seq, 16)
    y = lax.rem(line, 4)
    xl = lax.div(line, 4)

    def dev(s, b=bat):
        return {"seq": s, "batch": b}

    def at_line(xx, yy):
        return (xx * 4 + yy) * 16 + me

    yp, ym, y2 = lax.rem(y + 1, 4), lax.rem(y + 3, 4), lax.rem(y + 2, 4)
    up, down = dev(at_line(xl, yp)), dev(at_line(xl, ym))
    x0, x1 = dev(at_line(1 - xl, y)), dev(at_line(1 - xl, y), 1 - bat)
    nxt, prv = dev(lax.rem(seq + 2, SEQ_DEV)), dev(lax.rem(seq + 126, SEQ_DEV))
    nxt8, prv8 = dev(lax.rem(seq + 16, SEQ_DEV)), dev(lax.rem(seq + 112, SEQ_DEV))
    mate = dev(seq + 1 - 2 * core)
    z0, z7 = dev(line * 16 + core), dev(line * 16 + 14 + core)

    def z_dev(d, c):
        return dev(line * 16 + lax.rem(z + d, 8) * 2 + c)

    def rc(src, dst, ss, rs, to):
        return pltpu.make_async_remote_copy(
            src_ref=src, dst_ref=dst, send_sem=ss, recv_sem=rs, device_id=to, device_id_type=MESH
        )

    def got(ref, rs):
        rc(ref, ref, s_m.at[0], rs, mate).wait_recv()

    def gone(ref, ss):
        rc(ref, ref, ss, r_m.at[0], mate).wait_send()

    sends = []

    def send(src, dst, ss, rs, to):
        copy = rc(src, dst, ss, rs, to)
        copy.start()
        sends.append(copy)

    barrier = pltpu.get_barrier_semaphore()

    def greet(to):
        pl.semaphore_signal(barrier, inc=1, device_id=to, device_id_type=MESH)

    @pl.loop(1, 8)
    def _(d):
        greet(z_dev(d, 0))
        greet(z_dev(d, 1))

    for to in (mate, up, down, x0, x1, nxt, prv, nxt8, prv8):
        greet(to)

    own = pl.ds(pl.multiple_of(core * TOK, TOK), TOK)
    local = [
        pltpu.make_async_copy(hid, H.at[own], s_loc.at[0]),
        pltpu.make_async_copy(
            wqkv.at[:, pl.ds(pl.multiple_of(1024 + 256 * core, 256), 256)],
            ZW.at[me, :, pl.ds(0, 256)],
            s_loc.at[1],
        ),
        pltpu.make_async_copy(
            wqkv.at[:, pl.ds(pl.multiple_of(1536 + 256 * core, 256), 256)],
            ZW.at[me, :, pl.ds(256, 256)],
            s_loc.at[2],
        ),
        pltpu.make_async_copy(
            wqkv.at[:, pl.ds(pl.multiple_of(512 * core, 512), 512)], ZQ.at[me], s_loc.at[3]
        ),
        pltpu.make_async_copy(
            wout.at[:, pl.ds(pl.multiple_of(1152 * core, 128), 1152)], ZO.at[me], s_loc.at[4]
        ),
        pltpu.make_async_copy(seg, SEGW.at[16 + me], s_loc.at[5]),
    ]
    for copy in local:
        copy.start()

    pl.semaphore_wait(barrier, 23)

    def z_copies(p, c, to):
        if p == 0:
            src, dst = wqkv.at[:, pl.ds(pl.multiple_of(1024 + 256 * c, 256), 256)], ZW.at[me, :, pl.ds(0, 256)]
        elif p == 1:
            src, dst = wqkv.at[:, pl.ds(pl.multiple_of(1536 + 256 * c, 256), 256)], ZW.at[me, :, pl.ds(256, 256)]
        elif p == 2:
            src, dst = wqkv.at[:, pl.ds(pl.multiple_of(512 * c, 512), 512)], ZQ.at[me]
        else:
            src, dst = wout.at[:, pl.ds(pl.multiple_of(1152 * c, 128), 1152)], ZO.at[me]
        return rc(src, dst, s_z.at[p], r_z.at[p], to)

    def z_send(*pieces):
        for d in (1, 7, 2, 6):
            for c in (0, 1):
                for p in pieces:
                    z_copies(p, c, z_dev(d, c)).start()

        for p in pieces:
            z_copies(p, other, mate).start()

    def z_near(p):
        if p == 0:
            return ZW.at[pl.ds(0, 9), :, pl.ds(0, 256)]
        if p == 1:
            return ZW.at[pl.ds(0, 9), :, pl.ds(256, 256)]
        return ZQ.at[pl.ds(0, 9)] if p == 2 else ZO.at[pl.ds(0, 9)]

    def z_got(*pieces):
        for p in pieces:
            got(z_near(p), r_z.at[p])

    def z_forward(k):
        Z = (ZW, ZQ, ZO)[k]

        def on(d, to, cols=None):
            slots = pl.ds(lax.rem(z + d, 8) * 2, 2)
            ref = Z.at[slots] if cols is None else Z.at[slots, :, cols]
            rc(ref, ref, s_f.at[k], r_f.at[k], z_dev(to, core)).start()

        on(1, 6)
        on(7, 2)
        if k == 2:
            on(2, 6)
        else:
            on(2, 6, pl.ds(0, 256))
            on(6, 2, pl.ds(256, 256))

    def z_far(k):
        return (ZW, ZQ, ZO)[k].at[pl.ds(0, 6)]

    def seg_copy(to):
        return rc(seg, SEGW.at[16 + me], s_m.at[5], r_m.at[5], to)

    z_send(0, 1)
    send(hid, H.at[own], s_m.at[1], r_m.at[1], mate)

    @pl.loop(1, 8)
    def _(d):
        for c in (0, 1):
            seg_copy(z_dev(d, c)).start()

    seg_copy(mate).start()

    def norm_rows(first):
        @pl.loop(0, TOK // 64)
        def _(i):
            rows = pl.ds(pl.multiple_of(first + i * 64, 64), 64)
            v = H[rows, :].astype(F32)
            v = v * lax.rsqrt(jnp.mean(v * v, axis=-1, keepdims=True) + EPS) * pre[...]
            v = v.astype(BF)
            N[0, rows, :] = v[:, : D // 2]
            N[1, rows, :] = v[:, D // 2 :]

    for i in range(D // 128):
        pre[:, pl.ds(128 * i, 128)] = pre18[pl.ds(i, 1), :]
        post[:, pl.ds(128 * i, 128)] = post18[pl.ds(i, 1), :]
    local[0].wait()
    norm_rows(core * TOK)
    theirs = pl.ds(pl.multiple_of(other * TOK, TOK), TOK)
    got(H.at[theirs], r_m.at[1])
    norm_rows(other * TOK)

    @pl.loop(0, CHIP // 64)
    def _(i):
        rows = pl.ds(pl.multiple_of(i * 64, 64), 64)
        places = lax.div(seq, 2) * CHIP + i * 64 + lax.broadcasted_iota(I32, (64, HEAD // 2), 0)
        angles = places.astype(F32) * inverse[...]
        cos[rows, :] = jnp.cos(angles)
        sin[rows, :] = jnp.sin(angles)

    def part(s, yy, half, xx=xl):
        ln = xx * 4 + yy
        n = OROWS if s == 2 else LROWS
        first, size = (0, n) if half is None else (half * (n // 2), n // 2)
        rows = pl.ds(pl.multiple_of(ln * n + first, 16), size)
        if s == 2:
            return WO.at[core, rows, :]
        return W.at[rows, pl.ds(512 * s, 512)]

    def to_y(s, yy, half, to, k):
        ref = part(s, yy, half)
        rc(ref, ref, s_y.at[s], r_y.at[s, k], to).start()

    meet = jnp.where((lax.rem(y, 3) == 0) & (lax.rem(z, 7) == 0), 1, 0)
    x0_out = dev(at_line(1 - xl, y), bat + meet * (1 - 2 * bat))

    def to_x(s, yy, half):
        ref = part(s, yy, half)
        if s < 2:
            rc(ref, ref, s_x.at[s], r_x.at[s], x1 if half else x0).start()
        else:
            rc(ref, ref, s_x.at[s], r_x.at[2 + yy], x1 if half else x0_out).start()
            rc(ref, ref, s_m.at[3], r_m.at[3], mate).start()

    def across(yy):
        ref = part(2, yy, None, 1 - xl)
        got(ref, r_x.at[2 + yy])
        rc(ref, ref, s_m.at[3], r_m.at[3], mate).start()

    def stage1_up(s):
        to_y(s, y, 0, up, 0)
        to_y(s, y, 1, up, 1)

    def stage1(s):
        to_y(s, y, 1, down, 3)
        to_y(s, y, 0, down, 2)
        to_x(s, y, 0)
        to_x(s, y, 1)

    def from_below(s, half):
        got(part(s, ym, half), r_y.at[s, half])
        if s == 0 and half == 0:
            to_y(s, ym, 0, up, 4)
        to_x(s, ym, half)

    def from_above(s, half):
        got(part(s, yp, half), r_y.at[s, 2 + half])
        if s > 0 or half == 1:
            to_y(s, yp, half, down, 4 + half)
        to_x(s, yp, half)

    def stage2_up(s):
        from_below(s, 0)
        from_below(s, 1)

    def stage2(s):
        from_above(s, 1)
        from_above(s, 0)

    def from_second(s, half):
        got(part(s, y2, half), r_y.at[s, 4 + half])
        to_x(s, y2, half)

    def stage3(s):
        from_second(s, 0)
        from_second(s, 1)

    def stage4(s):
        first = pl.multiple_of((1 - xl) * (D // 2), 16)
        got(W.at[pl.ds(first, D // 2), pl.ds(512 * s, 512)], r_x.at[s])

    def streams_gone(s):
        n = OROWS if s == 2 else LROWS
        for rows, sem in ((3 * n, s_y.at[s]), (4 * n, s_x.at[s])):
            if s == 2:
                gone(WO.at[core, pl.ds(0, rows), :], sem)
            else:
                gone(W.at[pl.ds(0, rows), pl.ds(512 * s, 512)], sem)

    def repack(Z, col):
        for j in range(16):
            FS[pl.ds(18 * j, 18), :] = Z[j].astype(F32)
        W[pl.ds(pl.multiple_of(line * LROWS, 16), LROWS), pl.ds(col, 512)] = FS[...].astype(BF)

    z_got(0, 1)
    z_forward(0)
    got(z_far(0), r_f.at[0])
    local[1].wait()
    local[2].wait()
    repack(ZW, 0)
    stage1_up(0)
    stage1(0)
    z_send(2)
    from_below(0, 0)
    from_above(0, 1)
    z_got(2)
    z_forward(1)
    from_below(0, 1)
    from_above(0, 0)
    z_send(3)
    stage3(0)
    got(z_far(1), r_f.at[1])
    local[3].wait()
    repack(ZQ, 512)
    stage1_up(1)
    stage1(1)

    def project_half(col, xx, add, i):
        rows = pl.ds(i * TOK, TOK)
        w = W[pl.ds(pl.multiple_of(xx * (D // 2), 16), D // 2), pl.ds(col, 512)]
        term = jnp.dot(N[xx, rows, :], w, preferred_element_type=F32)
        ACC[rows, :] = ACC[rows, :] + term if add else term

    def project(col, xx, add):
        for i in (0, 1):
            project_half(col, xx, add, i)

    def turned(rows, col):
        a, b = ACC[rows, pl.ds(col, 128)], ACC[rows, pl.ds(col + 128, 128)]
        c, s = cos[rows, :], sin[rows, :]
        return (a * c - b * s).astype(BF), (b * c + a * s).astype(BF)

    project(0, xl, False)

    got(SEGW.at[pl.ds(16, 15)], r_m.at[5])
    local[5].wait()
    send(SEGW.at[pl.ds(16, 16)], SEGW.at[pl.ds(0, 16)], s_m.at[2], r_m.at[2], nxt8)
    for half in (0, 1):
        row = SEGW[16 + 2 * z + half].astype(F32)
        QS[pl.ds(half * TOK, TOK), :] = jnp.broadcast_to(row, (TOK, TOK)).T

    z_got(3)
    z_forward(2)
    stage4(0)
    project(0, 1 - xl, True)
    for half, buf in ((1, B), (0, A)):
        rows = pl.ds(half * TOK, TOK)
        low, high = turned(rows, 0)
        buf[0, 0, :, pl.ds(0, 128)] = low
        buf[0, 0, :, pl.ds(128, 128)] = high
        buf[0, 1] = ACC[rows, pl.ds(256, 256)].astype(BF)

    def piece(buf, t, c):
        return buf.at[t, c // 2, pl.ds(c % 2 * 128, 128), :]

    def stop(buf, k, c):
        return buf.at[k, c // 2, pl.ds(c % 2 * 128, 128), :]

    def pass_on(buf, t, u, c, ss, rs, to):
        rc(piece(buf, t, c), piece(buf, u, c), ss, rs.at[u, c], to).start()

    def pass_a(j, c):
        around = (z == 7) & (core == 1)

        @pl.when(jnp.logical_not(around))
        def _():
            pass_on(A, j, j + 1, c, s_a.at[0], r_a, nxt)

        @pl.when(around)
        def _():
            rc(piece(A, j, c), stop(RA, j, c), s_a.at[0], r_d.at[j, c], nxt8).start()

    def pass_b(j, c):
        t = 9 - j
        around = (z == 0) & (core == 1)

        @pl.when(jnp.logical_not(around))
        def _():
            pass_on(B, t, t - 1, c, s_b.at[0], r_b, prv)

        @pl.when(around)
        def _():
            rc(piece(B, t, c), stop(RB, j - 1, c), s_b.at[0], r_d.at[j - 1, c], prv8).start()

    def take_a(e):
        j, c = divmod(e, 4)
        if 1 <= j <= 8:
            got(piece(A, j, c), r_a.at[j, c])
        if 1 <= j <= 6:
            pass_a(j, c)

    def take_b(e):
        j, c = divmod(e, 4)
        if 1 <= j <= 8:
            got(piece(B, 9 - j, c), r_b.at[9 - j, c])
        if 1 <= j <= 7:
            pass_b(j, c)

    def help_a(e):
        j, c = divmod(e, 4)
        if 0 <= j <= 6:
            ref = stop(RA, j, c)
            got(ref, r_d.at[j, c])
            rc(ref, piece(A, j + 1, c), s_d.at[0], r_a.at[j + 1, c], z0).start()

    def help_b(e):
        j, c = divmod(e, 4)
        if 1 <= j <= 7:
            ref = stop(RB, j - 1, c)
            got(ref, r_d.at[j - 1, c])
            rc(ref, piece(B, 8 - j, c), s_d.at[0], r_b.at[8 - j, c], z7).start()

    def relay(e):
        for c in (0, 1):
            @pl.when((z == 0) & (core == c))
            def _():
                take_b(e)
                if c:
                    help_b(e - LAGS[2])
                take_a(e - LAGS[c])

            @pl.when((z == 7) & (core == c))
            def _():
                take_a(e)
                if c:
                    help_a(e - LAGS[2])
                take_b(e - LAGS[c])

        @pl.when((z > 0) & (z < 4))
        def _():
            take_b(e)
            take_a(e)

        @pl.when((z > 3) & (z < 7))
        def _():
            take_a(e)
            take_b(e)

    for c in range(4):
        pass_on(B, 0, 8, c, s_b.at[1], r_b, nxt8)
        pass_a(0, c)

    def attend(j, part):
        blocks = ((A, 0, 0), (B, 0, 1)) if j == 0 else ((A, j, 0), (B, 9 - j, 1))
        docs, firsts = [], []
        for _, t, half in blocks:
            index = 16 + 2 * z + half - 2 * t
            shut = jnp.logical_and(index < 16, line == 0)
            docs.append(jnp.where(shut, -1.0, SEGW[index].astype(F32)))
            firsts.append(half * TOK - CHIP * t)

        @pl.loop(2 * part, 2 * part + 2, unroll=2)
        def _(r):
            rows = pl.ds(pl.multiple_of(r * TOK, TOK), TOK)
            tok = pl.multiple_of(lax.rem(r, 2) * TOK, TOK)
            queries, whose = QQ[rows, :], QS[pl.ds(tok, TOK), :]
            sums, mixed = None, None
            for (buf, t, _), doc, first in zip(blocks, docs, firsts):
                s = lax.dot_general(
                    queries, buf[t, 0], (((1,), (1,)), ((), ())), preferred_element_type=F32
                )
                w = jnp.exp2(jnp.tanh(s * (1.0 / (16.0 * CAP))) * (CAP * LOG2E))
                allowed = whose == doc
                if t in (0, 8):
                    behind = (
                        lax.broadcasted_iota(I32, (TOK, TOK), 0)
                        - lax.broadcasted_iota(I32, (TOK, TOK), 1)
                        + (tok - first)
                    )
                    allowed &= (behind >= 0) & (behind < WINDOW)
                w = jnp.where(allowed, w, 0.0)
                part_sum = w[:, :128] + w[:, 128:]
                term = jnp.dot(w.astype(BF), buf[t, 1], preferred_element_type=F32)
                sums = part_sum if sums is None else sums + part_sum
                mixed = term if mixed is None else mixed + term
            if j == 0:
                L[rows, :] = sums
                O[rows, :] = mixed
            else:
                L[rows, :] += sums
                O[rows, :] += mixed

    def relay_and(e):
        relay(e)
        for action in extra.get(e, ()):
            action()

    def relays(first, last):
        for e in range(first, last):
            relay_and(e)

    eighth = [lambda c=c: pass_on(A, 0, 8, c, s_a.at[1], r_a, nxt8) for c in range(4)]
    extra = {
        11: [lambda: to_y(2, y, 0, up, 0)],
        12: [lambda: to_y(2, y, 1, down, 3)],
        14: [lambda: to_y(2, y, 1, up, 1)],
        16: [lambda: to_y(2, y, 0, down, 2), lambda: to_x(2, y, 0), lambda: to_x(2, y, 1)],
        17: [eighth[0]],
        18: [lambda: from_above(2, 1)],
        19: [eighth[1]],
        20: [lambda: from_below(2, 0)],
        21: [eighth[2]],
        22: [lambda: from_above(2, 0)],
        23: [eighth[3]],
        24: [lambda: from_below(2, 1)],
        27: [lambda: from_second(2, 1)],
        29: [lambda: from_second(2, 0)],
        25: [lambda: across(y)],
        28: [lambda: across(yp)],
        30: [lambda: across(ym)],
        34: [lambda: across(y2)],
    }

    relays(3, 8)
    stage2(1)

    got(z_far(2), r_f.at[2])
    local[4].wait()
    for j in range(0, 16, 2):
        pair = jnp.concatenate([ZO[j].astype(F32), ZO[j + 1].astype(F32)], axis=0)
        WO[core, pl.ds(pl.multiple_of(line * OROWS + 8 * j, 16), 16), :] = pair.astype(BF)

    gone(SEGW.at[pl.ds(0, 15)], s_m.at[5])
    for p in range(4):
        gone(z_near(p), s_z.at[p])
    for k in range(3):
        gone(z_far(k), s_f.at[k])

    relays(8, 12)
    stage2_up(1)
    stage3(1)
    def queries_of(half):
        rows = pl.ds(half * TOK, TOK)
        for h in (0, 1):
            low, high = turned(rows, 256 * h)
            dst = pl.ds(h * CHIP + half * TOK, TOK)
            QQ[dst, pl.ds(0, 128)] = low
            QQ[dst, pl.ds(128, 128)] = high

    relays(12, Q_AT - 4)
    for half in (0, 1):
        relay_and(Q_AT - 4 + half)
        project_half(512, xl, False, half)
    relay_and(Q_AT - 2)
    stage4(1)
    project_half(512, 1 - xl, True, 0)
    queries_of(0)
    relay_and(Q_AT - 1)
    project_half(512, 1 - xl, True, 1)
    queries_of(1)
    got(SEGW.at[pl.ds(0, 16)], r_m.at[2])

    todo = [(j, p) for j in range(9) for p in (0, 1)]
    for e in range(Q_AT, 36 + LAG):
        relays(e, e + 1)
        for _ in range(1 if e % 2 else 2):
            if todo and 4 * todo[0][0] + 3 + LAG <= e:
                attend(*todo.pop(0))
    for j, p in todo:
        attend(j, p)

    def attended(half, put):
        for h in (0, 1):
            rows = pl.ds(pl.multiple_of(h * CHIP + half * TOK, TOK), TOK)
            share = 1.0 / jnp.sum(L[rows, :], axis=-1, keepdims=True)
            put(h, (O[rows, :] * share).astype(BF))

    def put_other(h, value):
        SB[:, pl.ds(h * HEAD, HEAD)] = value

    def put_own(h, value):
        ATT[core, :, pl.ds(h * HEAD, HEAD)] = value

    attended(other, put_other)
    send(SB, ATT.at[core], s_m.at[4], r_m.at[4], mate)
    attended(core, put_own)
    got(WO.at[other], r_m.at[3])

    def branch(g, add):
        for c in (0, 1):
            cols = pl.ds(c * (D // 2), D // 2)
            weights = WO[c, pl.ds(pl.multiple_of(g * 512, 512), 512), :]
            term = jnp.dot(ATT[g], weights, preferred_element_type=F32)
            BR[:, cols] = BR[:, cols] + term if add else term

    branch(core, False)
    got(ATT.at[other], r_m.at[4])
    branch(other, True)

    @pl.loop(0, TOK // 32, unroll=2)
    def _(i):
        rows = pl.ds(pl.multiple_of(i * 32, 32), 32)
        v = BR[rows, :]
        v = v * lax.rsqrt(jnp.mean(v * v, axis=-1, keepdims=True) + EPS) * post[...]
        x = H[pl.ds(pl.multiple_of(core * TOK + i * 32, 32), 32), :].astype(F32)
        out[rows, :] = (x + v).astype(BF)

    for copy in sends:
        copy.wait_send()
    for buf, sem in ((A, s_a), (B, s_b)):
        gone(buf.at[pl.ds(0, 7)], sem.at[0])
        gone(buf.at[0], sem.at[1])
    @pl.when((lax.rem(z, 7) == 0) & (core == 1))
    def _():
        gone(A.at[pl.ds(0, 7)], s_d.at[0])

    for stream in range(3):
        streams_gone(stream)
    gone(WO.at[core], s_m.at[3])


def per_device(hidden_in, segment_ids, pre_gain, w_qkv, w_out, post_gain):
    inverse = np.float32(1.0) / np.float32(10000.0) ** (np.arange(HEAD // 2, dtype=np.float32) * 2 / HEAD)
    hbm = pl.BlockSpec(memory_space=pltpu.HBM)
    vmem = pl.BlockSpec(memory_space=pltpu.VMEM)
    dma = pltpu.SemaphoreType.DMA
    result = pl.pallas_call(
        kernel,
        out_shape=pltpu.VMEM((TOK, D), BF),
        in_specs=[hbm] * 4 + [vmem] * 3,
        out_specs=vmem,
        scratch_shapes=[
            pltpu.VMEM((CHIP, HEAD // 2), F32),
            pltpu.VMEM((CHIP, HEAD // 2), F32),
            pltpu.VMEM((1, D), F32),
            pltpu.VMEM((1, D), F32),
            pltpu.VMEM((CHIP, D), BF),
            pltpu.VMEM((2, CHIP, D // 2), BF),
            pltpu.VMEM((D, 1024), BF),
            pltpu.VMEM((2, 1024, D // 2), BF),
            pltpu.VMEM((16, 18, 512), BF),
            pltpu.VMEM((16, 18, 512), BF),
            pltpu.VMEM((16, 8, D // 2), BF),
            pltpu.VMEM((LROWS, 512), F32),
            pltpu.VMEM((CHIP, 512), F32),
            pltpu.VMEM((2 * CHIP, HEAD), BF),
            pltpu.VMEM((2 * CHIP, HEAD), F32),
            pltpu.VMEM((2 * CHIP, 128), F32),
            pltpu.VMEM((9, 2, TOK, HEAD), BF),
            pltpu.VMEM((9, 2, TOK, HEAD), BF),
            pltpu.VMEM((7, 2, TOK, HEAD), BF),
            pltpu.VMEM((7, 2, TOK, HEAD), BF),
            pltpu.VMEM((32, 1, TOK), I32),
            pltpu.VMEM((CHIP, TOK), F32),
            pltpu.VMEM((2, TOK, 512), BF),
            pltpu.VMEM((TOK, 512), BF),
            pltpu.VMEM((TOK, D), F32),
            dma((6,)),
            dma((4,)), dma((4,)),
            dma((3,)), dma((3,)),
            dma((3,)), dma((3, 6)),
            dma((3,)), dma((6,)),
            dma((2,)), dma((9, 4)),
            dma((2,)), dma((9, 4)),
            dma((1,)), dma((7, 4)),
            dma((6,)), dma((6,)),
        ],
        compiler_params=pltpu.CompilerParams(
            collective_id=0, has_side_effects=True, vmem_limit_bytes=60 * 1024 * 1024
        ),
    )(
        hidden_in[0],
        segment_ids,
        w_qkv,
        w_out,
        jnp.asarray(inverse.astype(np.float32).reshape(1, HEAD // 2)),
        pre_gain.reshape(D // 128, 128),
        post_gain.reshape(D // 128, 128),
    )
    return result[None]


def solution(mesh):
    placed = (P("batch", "seq", None), P("batch", "seq"), P(), P("seq", None), P("seq", None), P())
    return jax.shard_map(
        per_device, mesh=mesh, in_specs=placed, out_specs=P("batch", "seq", None), check_vma=False
    )
```

```python
import jax
import jax.numpy as jnp
import numpy as np
from jax import lax
from jax.experimental import pallas as pl
from jax.experimental.pallas import tpu as pltpu
from jax.sharding import PartitionSpec as P

MESH = pl.DeviceIdType.MESH
BF, F32, I32 = jnp.bfloat16, jnp.float32, jnp.int32

D = 2304
HEAD = 256
WINDOW = 4096
TOK = 256
CHIP = 512
SEQ_DEV = 128
LINES = 8
LROWS = 288
OROWS = 128
LAGS = (2, 4, 3)
LAG = max(LAGS)
Q_AT = 19
EPS = 1e-06
CAP = 50.0
LOG2E = 1.4426950408889634


def kernel(
    hid, seg, wqkv, wout, inverse, pre18, post18, out,
    cos, sin, pre, post, H, N, W, WO, ZW, ZQ, ZO, FS, ACC, QQ, O, L, A, B, RA, RB, SEGW, QS, ATT, SB, BR,
    s_loc, s_z, r_z, s_f, r_f, s_y, r_y, s_x, r_x, s_a, r_a, s_b, r_b, s_d, r_d, s_m, r_m,
):
    seq = lax.axis_index("seq")
    bat = lax.axis_index("batch")
    core = lax.rem(seq, 2)
    other = 1 - core
    me = lax.rem(seq, 16)
    z = lax.div(me, 2)
    line = lax.div(seq, 16)
    y = lax.rem(line, 4)
    xl = lax.div(line, 4)

    def dev(s, b=bat):
        return {"seq": s, "batch": b}

    def at_line(xx, yy):
        return (xx * 4 + yy) * 16 + me

    yp, ym, y2 = lax.rem(y + 1, 4), lax.rem(y + 3, 4), lax.rem(y + 2, 4)
    up, down = dev(at_line(xl, yp)), dev(at_line(xl, ym))
    x0, x1 = dev(at_line(1 - xl, y)), dev(at_line(1 - xl, y), 1 - bat)
    nxt, prv = dev(lax.rem(seq + 2, SEQ_DEV)), dev(lax.rem(seq + 126, SEQ_DEV))
    nxt8, prv8 = dev(lax.rem(seq + 16, SEQ_DEV)), dev(lax.rem(seq + 112, SEQ_DEV))
    mate = dev(seq + 1 - 2 * core)
    z0, z7 = dev(line * 16 + core), dev(line * 16 + 14 + core)

    def z_dev(d, c):
        return dev(line * 16 + lax.rem(z + d, 8) * 2 + c)

    def rc(src, dst, ss, rs, to):
        return pltpu.make_async_remote_copy(
            src_ref=src, dst_ref=dst, send_sem=ss, recv_sem=rs, device_id=to, device_id_type=MESH
        )

    def got(ref, rs):
        rc(ref, ref, s_m.at[0], rs, mate).wait_recv()

    def gone(ref, ss):
        rc(ref, ref, ss, r_m.at[0], mate).wait_send()

    sends = []

    def send(src, dst, ss, rs, to):
        copy = rc(src, dst, ss, rs, to)
        copy.start()
        sends.append(copy)

    barrier = pltpu.get_barrier_semaphore()

    def greet(to):
        pl.semaphore_signal(barrier, inc=1, device_id=to, device_id_type=MESH)

    @pl.loop(1, 8)
    def _(d):
        greet(z_dev(d, 0))
        greet(z_dev(d, 1))

    for to in (mate, up, down, x0, x1, nxt, prv, nxt8, prv8):
        greet(to)

    own = pl.ds(pl.multiple_of(core * TOK, TOK), TOK)
    local = [
        pltpu.make_async_copy(hid, H.at[own], s_loc.at[0]),
        pltpu.make_async_copy(
            wqkv.at[:, pl.ds(pl.multiple_of(1024 + 256 * core, 256), 256)],
            ZW.at[me, :, pl.ds(0, 256)],
            s_loc.at[1],
        ),
        pltpu.make_async_copy(
            wqkv.at[:, pl.ds(pl.multiple_of(1536 + 256 * core, 256), 256)],
            ZW.at[me, :, pl.ds(256, 256)],
            s_loc.at[2],
        ),
        pltpu.make_async_copy(
            wqkv.at[:, pl.ds(pl.multiple_of(512 * core, 512), 512)], ZQ.at[me], s_loc.at[3]
        ),
        pltpu.make_async_copy(
            wout.at[:, pl.ds(pl.multiple_of(1152 * core, 128), 1152)], ZO.at[me], s_loc.at[4]
        ),
        pltpu.make_async_copy(seg, SEGW.at[16 + me], s_loc.at[5]),
    ]
    for copy in local:
        copy.start()

    pl.semaphore_wait(barrier, 23)

    def z_copies(p, c, to):
        if p == 0:
            src, dst = wqkv.at[:, pl.ds(pl.multiple_of(1024 + 256 * c, 256), 256)], ZW.at[me, :, pl.ds(0, 256)]
        elif p == 1:
            src, dst = wqkv.at[:, pl.ds(pl.multiple_of(1536 + 256 * c, 256), 256)], ZW.at[me, :, pl.ds(256, 256)]
        elif p == 2:
            src, dst = wqkv.at[:, pl.ds(pl.multiple_of(512 * c, 512), 512)], ZQ.at[me]
        else:
            src, dst = wout.at[:, pl.ds(pl.multiple_of(1152 * c, 128), 1152)], ZO.at[me]
        return rc(src, dst, s_z.at[p], r_z.at[p], to)

    def z_send(*pieces):
        for d in (1, 7, 2, 6):
            for c in (0, 1):
                for p in pieces:
                    z_copies(p, c, z_dev(d, c)).start()

        for p in pieces:
            z_copies(p, other, mate).start()

    def z_near(p):
        if p == 0:
            return ZW.at[pl.ds(0, 9), :, pl.ds(0, 256)]
        if p == 1:
            return ZW.at[pl.ds(0, 9), :, pl.ds(256, 256)]
        return ZQ.at[pl.ds(0, 9)] if p == 2 else ZO.at[pl.ds(0, 9)]

    def z_got(*pieces):
        for p in pieces:
            got(z_near(p), r_z.at[p])

    def z_forward(k):
        Z = (ZW, ZQ, ZO)[k]

        def on(d, to, cols=None):
            slots = pl.ds(lax.rem(z + d, 8) * 2, 2)
            ref = Z.at[slots] if cols is None else Z.at[slots, :, cols]
            rc(ref, ref, s_f.at[k], r_f.at[k], z_dev(to, core)).start()

        on(1, 6)
        on(7, 2)
        if k == 2:
            on(2, 6)
        else:
            on(2, 6, pl.ds(0, 256))
            on(6, 2, pl.ds(256, 256))

    def z_far(k):
        return (ZW, ZQ, ZO)[k].at[pl.ds(0, 6)]

    def seg_copy(to):
        return rc(seg, SEGW.at[16 + me], s_m.at[5], r_m.at[5], to)

    z_send(0, 1)
    send(hid, H.at[own], s_m.at[1], r_m.at[1], mate)

    @pl.loop(1, 8)
    def _(d):
        for c in (0, 1):
            seg_copy(z_dev(d, c)).start()

    seg_copy(mate).start()

    def norm_rows(first):
        @pl.loop(0, TOK // 64)
        def _(i):
            rows = pl.ds(pl.multiple_of(first + i * 64, 64), 64)
            v = H[rows, :].astype(F32)
            v = v * lax.rsqrt(jnp.mean(v * v, axis=-1, keepdims=True) + EPS) * pre[...]
            v = v.astype(BF)
            N[0, rows, :] = v[:, : D // 2]
            N[1, rows, :] = v[:, D // 2 :]

    for i in range(D // 128):
        pre[:, pl.ds(128 * i, 128)] = pre18[pl.ds(i, 1), :]
        post[:, pl.ds(128 * i, 128)] = post18[pl.ds(i, 1), :]
    local[0].wait()
    norm_rows(core * TOK)
    theirs = pl.ds(pl.multiple_of(other * TOK, TOK), TOK)
    got(H.at[theirs], r_m.at[1])
    norm_rows(other * TOK)

    @pl.loop(0, CHIP // 64)
    def _(i):
        rows = pl.ds(pl.multiple_of(i * 64, 64), 64)
        places = lax.div(seq, 2) * CHIP + i * 64 + lax.broadcasted_iota(I32, (64, HEAD // 2), 0)
        angles = places.astype(F32) * inverse[...]
        cos[rows, :] = jnp.cos(angles)
        sin[rows, :] = jnp.sin(angles)

    def part(s, yy, half, xx=xl):
        ln = xx * 4 + yy
        n = OROWS if s == 2 else LROWS
        first, size = (0, n) if half is None else (half * (n // 2), n // 2)
        rows = pl.ds(pl.multiple_of(ln * n + first, 16), size)
        if s == 2:
            return WO.at[core, rows, :]
        return W.at[rows, pl.ds(512 * s, 512)]

    def to_y(s, yy, half, to, k):
        ref = part(s, yy, half)
        rc(ref, ref, s_y.at[s], r_y.at[s, k], to).start()

    meet = jnp.where((lax.rem(y, 3) == 0) & (lax.rem(z, 7) == 0), 1, 0)
    x0_out = dev(at_line(1 - xl, y), bat + meet * (1 - 2 * bat))

    def to_x(s, yy, half):
        ref = part(s, yy, half)
        if s < 2:
            rc(ref, ref, s_x.at[s], r_x.at[s], x1 if half else x0).start()
        else:
            rc(ref, ref, s_x.at[s], r_x.at[2 + yy], x1 if half else x0_out).start()
            rc(ref, ref, s_m.at[3], r_m.at[3], mate).start()

    def across(yy):
        ref = part(2, yy, None, 1 - xl)
        got(ref, r_x.at[2 + yy])
        rc(ref, ref, s_m.at[3], r_m.at[3], mate).start()

    def stage1_up(s):
        to_y(s, y, 0, up, 0)
        to_y(s, y, 1, up, 1)

    def stage1(s):
        to_y(s, y, 1, down, 3)
        to_y(s, y, 0, down, 2)
        to_x(s, y, 0)
        to_x(s, y, 1)

    def from_below(s, half):
        got(part(s, ym, half), r_y.at[s, half])
        if s == 0 and half == 0:
            to_y(s, ym, 0, up, 4)
        to_x(s, ym, half)

    def from_above(s, half):
        got(part(s, yp, half), r_y.at[s, 2 + half])
        if s > 0 or half == 1:
            to_y(s, yp, half, down, 4 + half)
        to_x(s, yp, half)

    def stage2_up(s):
        from_below(s, 0)
        from_below(s, 1)

    def stage2(s):
        from_above(s, 1)
        from_above(s, 0)

    def from_second(s, half):
        got(part(s, y2, half), r_y.at[s, 4 + half])
        to_x(s, y2, half)

    def stage3(s):
        from_second(s, 0)
        from_second(s, 1)

    def stage4(s):
        first = pl.multiple_of((1 - xl) * (D // 2), 16)
        got(W.at[pl.ds(first, D // 2), pl.ds(512 * s, 512)], r_x.at[s])

    def streams_gone(s):
        n = OROWS if s == 2 else LROWS
        for rows, sem in ((3 * n, s_y.at[s]), (4 * n, s_x.at[s])):
            if s == 2:
                gone(WO.at[core, pl.ds(0, rows), :], sem)
            else:
                gone(W.at[pl.ds(0, rows), pl.ds(512 * s, 512)], sem)

    def repack(Z, col):
        for j in range(16):
            FS[pl.ds(18 * j, 18), :] = Z[j].astype(F32)
        W[pl.ds(pl.multiple_of(line * LROWS, 16), LROWS), pl.ds(col, 512)] = FS[...].astype(BF)

    z_got(0, 1)
    z_forward(0)
    got(z_far(0), r_f.at[0])
    local[1].wait()
    local[2].wait()
    repack(ZW, 0)
    stage1_up(0)
    stage1(0)
    z_send(2)
    from_below(0, 0)
    from_above(0, 1)
    z_got(2)
    z_forward(1)
    from_below(0, 1)
    from_above(0, 0)
    z_send(3)
    stage3(0)
    got(z_far(1), r_f.at[1])
    local[3].wait()
    repack(ZQ, 512)
    stage1_up(1)
    stage1(1)

    def project_half(col, xx, add, i):
        rows = pl.ds(i * TOK, TOK)
        w = W[pl.ds(pl.multiple_of(xx * (D // 2), 16), D // 2), pl.ds(col, 512)]
        term = jnp.dot(N[xx, rows, :], w, preferred_element_type=F32)
        ACC[rows, :] = ACC[rows, :] + term if add else term

    def project(col, xx, add):
        for i in (0, 1):
            project_half(col, xx, add, i)

    def turned(rows, col):
        a, b = ACC[rows, pl.ds(col, 128)], ACC[rows, pl.ds(col + 128, 128)]
        c, s = cos[rows, :], sin[rows, :]
        return (a * c - b * s).astype(BF), (b * c + a * s).astype(BF)

    project(0, xl, False)

    got(SEGW.at[pl.ds(16, 15)], r_m.at[5])
    local[5].wait()
    send(SEGW.at[pl.ds(16, 16)], SEGW.at[pl.ds(0, 16)], s_m.at[2], r_m.at[2], nxt8)
    for half in (0, 1):
        row = SEGW[16 + 2 * z + half].astype(F32)
        QS[pl.ds(half * TOK, TOK), :] = jnp.broadcast_to(row, (TOK, TOK)).T

    z_got(3)
    z_forward(2)
    stage4(0)
    def own_block(half, buf):
        project_half(0, 1 - xl, True, half)
        rows = pl.ds(half * TOK, TOK)
        low, high = turned(rows, 0)
        buf[0, 0, :, pl.ds(0, 128)] = low
        buf[0, 0, :, pl.ds(128, 128)] = high
        buf[0, 1] = ACC[rows, pl.ds(256, 256)].astype(BF)

    def piece(buf, t, c):
        return buf.at[t, c // 2, pl.ds(c % 2 * 128, 128), :]

    def stop(buf, k, c):
        return buf.at[k, c // 2, pl.ds(c % 2 * 128, 128), :]

    def pass_on(buf, t, u, c, ss, rs, to):
        rc(piece(buf, t, c), piece(buf, u, c), ss, rs.at[u, c], to).start()

    def pass_a(j, c):
        around = (z == 7) & (core == 1)

        @pl.when(jnp.logical_not(around))
        def _():
            pass_on(A, j, j + 1, c, s_a.at[0], r_a, nxt)

        @pl.when(around)
        def _():
            rc(piece(A, j, c), stop(RA, j, c), s_a.at[0], r_d.at[j, c], nxt8).start()

    def pass_b(j, c):
        t = 9 - j
        around = (z == 0) & (core == 1)

        @pl.when(jnp.logical_not(around))
        def _():
            pass_on(B, t, t - 1, c, s_b.at[0], r_b, prv)

        @pl.when(around)
        def _():
            rc(piece(B, t, c), stop(RB, j - 1, c), s_b.at[0], r_d.at[j - 1, c], prv8).start()

    def take_a(e):
        j, c = divmod(e, 4)
        if 1 <= j <= 7:
            got(piece(A, j, c), r_a.at[j, c])
        if 1 <= j <= 6:
            pass_a(j, c)

    def take_b(e):
        j, c = divmod(e, 4)
        if 1 <= j <= 8:
            got(piece(B, 9 - j, c), r_b.at[9 - j, c])
        if 1 <= j <= 7:
            pass_b(j, c)

    def help_a(e):
        j, c = divmod(e, 4)
        if 0 <= j <= 6:
            ref = stop(RA, j, c)
            got(ref, r_d.at[j, c])
            rc(ref, piece(A, j + 1, c), s_d.at[0], r_a.at[j + 1, c], z0).start()

    def help_b(e):
        j, c = divmod(e, 4)
        if 1 <= j <= 7:
            ref = stop(RB, j - 1, c)
            got(ref, r_d.at[j - 1, c])
            rc(ref, piece(B, 8 - j, c), s_d.at[0], r_b.at[8 - j, c], z7).start()

    def relay(e):
        for c in (0, 1):
            @pl.when((z == 0) & (core == c))
            def _():
                take_b(e)
                if c:
                    help_b(e - LAGS[2])
                take_a(e - LAGS[c])

            @pl.when((z == 7) & (core == c))
            def _():
                take_a(e)
                if c:
                    help_a(e - LAGS[2])
                take_b(e - LAGS[c])

        @pl.when((z > 0) & (z < 4))
        def _():
            take_b(e)
            take_a(e)

        @pl.when((z > 3) & (z < 7))
        def _():
            take_a(e)
            take_b(e)

    own_block(1, B)
    for c in range(4):
        pass_on(B, 0, 8, c, s_b.at[1], r_b, nxt8)
    own_block(0, A)
    for c in range(4):
        pass_a(0, c)

    def attend(j, part):
        blocks = (
            ((A, 0, 0), (B, 0, 1)),
            *(((A, t, 0), (B, 9 - t, 1)) for t in range(1, 8)),
            ((B, 1, 1),),
            ((A, 8, 0),),
        )[j]
        docs, firsts = [], []
        for _, t, half in blocks:
            index = 16 + 2 * z + half - 2 * t
            shut = jnp.logical_and(index < 16, line == 0)
            docs.append(jnp.where(shut, -1.0, SEGW[index].astype(F32)))
            firsts.append(half * TOK - CHIP * t)

        @pl.loop(2 * part, 2 * part + 2, unroll=2)
        def _(r):
            rows = pl.ds(pl.multiple_of(r * TOK, TOK), TOK)
            tok = pl.multiple_of(lax.rem(r, 2) * TOK, TOK)
            queries, whose = QQ[rows, :], QS[pl.ds(tok, TOK), :]
            sums, mixed = None, None
            for (buf, t, _), doc, first in zip(blocks, docs, firsts):
                s = lax.dot_general(
                    queries, buf[t, 0], (((1,), (1,)), ((), ())), preferred_element_type=F32
                )
                w = jnp.exp2(jnp.tanh(s * (1.0 / (16.0 * CAP))) * (CAP * LOG2E))
                allowed = whose == doc
                if t in (0, 8):
                    behind = (
                        lax.broadcasted_iota(I32, (TOK, TOK), 0)
                        - lax.broadcasted_iota(I32, (TOK, TOK), 1)
                        + (tok - first)
                    )
                    allowed &= (behind >= 0) & (behind < WINDOW)
                w = jnp.where(allowed, w, 0.0)
                part_sum = w[:, :128] + w[:, 128:]
                term = jnp.dot(w.astype(BF), buf[t, 1], preferred_element_type=F32)
                sums = part_sum if sums is None else sums + part_sum
                mixed = term if mixed is None else mixed + term
            if j == 0:
                L[rows, :] = sums
                O[rows, :] = mixed
            else:
                L[rows, :] += sums
                O[rows, :] += mixed

    def relay_and(e):
        relay(e)
        for action in extra.get(e, ()):
            action()

    def relays(first, last):
        for e in range(first, last):
            relay_and(e)

    eighth = [lambda c=c: pass_on(A, 0, 8, c, s_a.at[1], r_a, nxt8) for c in range(4)]
    extra = {
        5: [lambda: from_above(1, 1)],
        7: [lambda: from_above(1, 0)],
        9: [lambda: from_below(1, 0)],
        10: [lambda: from_below(1, 1)],
        13: [lambda: from_second(1, 1), lambda: from_second(1, 0)],
        11: [lambda: to_y(2, y, 0, up, 0)],
        12: [lambda: to_y(2, y, 1, down, 3)],
        14: [lambda: to_y(2, y, 1, up, 1)],
        16: [lambda: to_y(2, y, 0, down, 2), lambda: to_x(2, y, 0), lambda: to_x(2, y, 1)],
        17: [eighth[0]],
        18: [lambda: from_above(2, 1)],
        19: [eighth[1]],
        20: [lambda: from_below(2, 0)],
        21: [eighth[2]],
        22: [lambda: from_above(2, 0)],
        23: [eighth[3]],
        24: [lambda: from_below(2, 1)],
        27: [lambda: from_second(2, 1)],
        29: [lambda: from_second(2, 0)],
        25: [lambda: across(y)],
        28: [lambda: across(yp)],
        30: [lambda: across(ym)],
        31: [lambda: [got(piece(A, 8, c), r_a.at[8, c]) for c in range(4)]],
        34: [lambda: across(y2)],
    }

    relays(3, 8)

    got(z_far(2), r_f.at[2])
    local[4].wait()
    for j in range(0, 16, 2):
        pair = jnp.concatenate([ZO[j].astype(F32), ZO[j + 1].astype(F32)], axis=0)
        WO[core, pl.ds(pl.multiple_of(line * OROWS + 8 * j, 16), 16), :] = pair.astype(BF)

    gone(SEGW.at[pl.ds(0, 15)], s_m.at[5])
    for p in range(4):
        gone(z_near(p), s_z.at[p])
    for k in range(3):
        gone(z_far(k), s_f.at[k])

    relays(8, 12)
    def queries_of(half):
        rows = pl.ds(half * TOK, TOK)
        for h in (0, 1):
            low, high = turned(rows, 256 * h)
            dst = pl.ds(h * CHIP + half * TOK, TOK)
            QQ[dst, pl.ds(0, 128)] = low
            QQ[dst, pl.ds(128, 128)] = high

    relays(12, Q_AT - 4)
    for half in (0, 1):
        relay_and(Q_AT - 4 + half)
        project_half(512, xl, False, half)
    relay_and(Q_AT - 2)
    stage4(1)
    project_half(512, 1 - xl, True, 0)
    queries_of(0)
    relay_and(Q_AT - 1)
    project_half(512, 1 - xl, True, 1)
    queries_of(1)
    got(SEGW.at[pl.ds(0, 16)], r_m.at[2])

    todo = [(j, p) for j in (0, 1, 2, 3, 4, 5, 6, 9, 7, 8) for p in (0, 1)]
    for e in range(Q_AT, 36 + LAG):
        relays(e, e + 1)
        for _ in range(1 if e % 2 else 2):
            if todo and (31 if todo[0][0] == 9 else 4 * todo[0][0] + 3 + LAG) <= e:
                attend(*todo.pop(0))
    for j, p in todo:
        attend(j, p)

    def attended(half, put):
        for h in (0, 1):
            rows = pl.ds(pl.multiple_of(h * CHIP + half * TOK, TOK), TOK)
            share = 1.0 / jnp.sum(L[rows, :], axis=-1, keepdims=True)
            put(h, (O[rows, :] * share).astype(BF))

    def put_other(h, value):
        SB[:, pl.ds(h * HEAD, HEAD)] = value

    def put_own(h, value):
        ATT[core, :, pl.ds(h * HEAD, HEAD)] = value

    attended(other, put_other)
    send(SB, ATT.at[core], s_m.at[4], r_m.at[4], mate)
    attended(core, put_own)
    got(WO.at[other], r_m.at[3])

    def branch(g, add):
        for c in (0, 1):
            cols = pl.ds(c * (D // 2), D // 2)
            weights = WO[c, pl.ds(pl.multiple_of(g * 512, 512), 512), :]
            term = jnp.dot(ATT[g], weights, preferred_element_type=F32)
            BR[:, cols] = BR[:, cols] + term if add else term

    branch(core, False)
    got(ATT.at[other], r_m.at[4])
    branch(other, True)

    @pl.loop(0, TOK // 32, unroll=2)
    def _(i):
        rows = pl.ds(pl.multiple_of(i * 32, 32), 32)
        v = BR[rows, :]
        v = v * lax.rsqrt(jnp.mean(v * v, axis=-1, keepdims=True) + EPS) * post[...]
        x = H[pl.ds(pl.multiple_of(core * TOK + i * 32, 32), 32), :].astype(F32)
        out[rows, :] = (x + v).astype(BF)

    for copy in sends:
        copy.wait_send()
    for buf, sem in ((A, s_a), (B, s_b)):
        gone(buf.at[pl.ds(0, 7)], sem.at[0])
        gone(buf.at[0], sem.at[1])
    @pl.when((lax.rem(z, 7) == 0) & (core == 1))
    def _():
        gone(A.at[pl.ds(0, 7)], s_d.at[0])

    for stream in range(3):
        streams_gone(stream)
    gone(WO.at[core], s_m.at[3])


def per_device(hidden_in, segment_ids, pre_gain, w_qkv, w_out, post_gain):
    inverse = np.float32(1.0) / np.float32(10000.0) ** (np.arange(HEAD // 2, dtype=np.float32) * 2 / HEAD)
    hbm = pl.BlockSpec(memory_space=pltpu.HBM)
    vmem = pl.BlockSpec(memory_space=pltpu.VMEM)
    dma = pltpu.SemaphoreType.DMA
    result = pl.pallas_call(
        kernel,
        out_shape=pltpu.VMEM((TOK, D), BF),
        in_specs=[hbm] * 4 + [vmem] * 3,
        out_specs=vmem,
        scratch_shapes=[
            pltpu.VMEM((CHIP, HEAD // 2), F32),
            pltpu.VMEM((CHIP, HEAD // 2), F32),
            pltpu.VMEM((1, D), F32),
            pltpu.VMEM((1, D), F32),
            pltpu.VMEM((CHIP, D), BF),
            pltpu.VMEM((2, CHIP, D // 2), BF),
            pltpu.VMEM((D, 1024), BF),
            pltpu.VMEM((2, 1024, D // 2), BF),
            pltpu.VMEM((16, 18, 512), BF),
            pltpu.VMEM((16, 18, 512), BF),
            pltpu.VMEM((16, 8, D // 2), BF),
            pltpu.VMEM((LROWS, 512), F32),
            pltpu.VMEM((CHIP, 512), F32),
            pltpu.VMEM((2 * CHIP, HEAD), BF),
            pltpu.VMEM((2 * CHIP, HEAD), F32),
            pltpu.VMEM((2 * CHIP, 128), F32),
            pltpu.VMEM((9, 2, TOK, HEAD), BF),
            pltpu.VMEM((9, 2, TOK, HEAD), BF),
            pltpu.VMEM((7, 2, TOK, HEAD), BF),
            pltpu.VMEM((7, 2, TOK, HEAD), BF),
            pltpu.VMEM((32, 1, TOK), I32),
            pltpu.VMEM((CHIP, TOK), F32),
            pltpu.VMEM((2, TOK, 512), BF),
            pltpu.VMEM((TOK, 512), BF),
            pltpu.VMEM((TOK, D), F32),
            dma((6,)),
            dma((4,)), dma((4,)),
            dma((3,)), dma((3,)),
            dma((3,)), dma((3, 6)),
            dma((3,)), dma((6,)),
            dma((2,)), dma((9, 4)),
            dma((2,)), dma((9, 4)),
            dma((1,)), dma((7, 4)),
            dma((6,)), dma((6,)),
        ],
        compiler_params=pltpu.CompilerParams(
            collective_id=0, has_side_effects=True, vmem_limit_bytes=60 * 1024 * 1024
        ),
    )(
        hidden_in[0],
        segment_ids,
        w_qkv,
        w_out,
        jnp.asarray(inverse.astype(np.float32).reshape(1, HEAD // 2)),
        pre_gain.reshape(D // 128, 128),
        post_gain.reshape(D // 128, 128),
    )
    return result[None]


def solution(mesh):
    placed = (P("batch", "seq", None), P("batch", "seq"), P(), P("seq", None), P("seq", None), P())
    return jax.shard_map(
        per_device, mesh=mesh, in_specs=placed, out_specs=P("batch", "seq", None), check_vma=False
    )
```

```python
import jax
import jax.numpy as jnp
import numpy as np
from jax import lax
from jax.experimental import pallas as pl
from jax.experimental.pallas import tpu as pltpu
from jax.sharding import PartitionSpec as P

MESH = pl.DeviceIdType.MESH
BF, F32, I32 = jnp.bfloat16, jnp.float32, jnp.int32

D = 2304
HEAD = 256
WINDOW = 4096
TOK = 256
CHIP = 512
SEQ_DEV = 128
LINES = 8
LROWS = 288
OROWS = 128
LAGS = (2, 4, 3)
LAG = max(LAGS)
Q_AT = 20
EPS = 1e-06
CAP = 50.0
LOG2E = 1.4426950408889634


def kernel(
    hid, seg, wqkv, wout, inverse, pre18, post18, out,
    cos, sin, pre, post, H, N, W, WO, ZW, ZQ, ZO, FS, ACC, QQ, O, L, A, B, RA, RB, SEGW, QS, ATT, SB, BR,
    s_loc, s_z, r_z, s_f, r_f, s_y, r_y, s_x, r_x, s_a, r_a, s_b, r_b, s_d, r_d, s_m, r_m,
):
    seq = lax.axis_index("seq")
    bat = lax.axis_index("batch")
    core = lax.rem(seq, 2)
    other = 1 - core
    me = lax.rem(seq, 16)
    z = lax.div(me, 2)
    line = lax.div(seq, 16)
    y = lax.rem(line, 4)
    xl = lax.div(line, 4)

    def dev(s, b=bat):
        return {"seq": s, "batch": b}

    def at_line(xx, yy):
        return (xx * 4 + yy) * 16 + me

    yp, ym, y2 = lax.rem(y + 1, 4), lax.rem(y + 3, 4), lax.rem(y + 2, 4)
    up, down = dev(at_line(xl, yp)), dev(at_line(xl, ym))
    x0, x1 = dev(at_line(1 - xl, y)), dev(at_line(1 - xl, y), 1 - bat)
    nxt, prv = dev(lax.rem(seq + 2, SEQ_DEV)), dev(lax.rem(seq + 126, SEQ_DEV))
    nxt8, prv8 = dev(lax.rem(seq + 16, SEQ_DEV)), dev(lax.rem(seq + 112, SEQ_DEV))
    mate = dev(seq + 1 - 2 * core)
    z0, z7 = dev(line * 16 + core), dev(line * 16 + 14 + core)

    def z_dev(d, c):
        return dev(line * 16 + lax.rem(z + d, 8) * 2 + c)

    def rc(src, dst, ss, rs, to):
        return pltpu.make_async_remote_copy(
            src_ref=src, dst_ref=dst, send_sem=ss, recv_sem=rs, device_id=to, device_id_type=MESH
        )

    def got(ref, rs):
        rc(ref, ref, s_m.at[0], rs, mate).wait_recv()

    def gone(ref, ss):
        rc(ref, ref, ss, r_m.at[0], mate).wait_send()

    sends = []

    def send(src, dst, ss, rs, to):
        copy = rc(src, dst, ss, rs, to)
        copy.start()
        sends.append(copy)

    barrier = pltpu.get_barrier_semaphore()

    def greet(to):
        pl.semaphore_signal(barrier, inc=1, device_id=to, device_id_type=MESH)

    @pl.loop(1, 8)
    def _(d):
        greet(z_dev(d, 0))
        greet(z_dev(d, 1))

    for to in (mate, up, down, x0, x1, nxt, prv, nxt8, prv8):
        greet(to)

    own = pl.ds(pl.multiple_of(core * TOK, TOK), TOK)
    local = [
        pltpu.make_async_copy(hid, H.at[own], s_loc.at[0]),
        pltpu.make_async_copy(
            wqkv.at[:, pl.ds(pl.multiple_of(1024 + 256 * core, 256), 256)],
            ZW.at[me, :, pl.ds(0, 256)],
            s_loc.at[1],
        ),
        pltpu.make_async_copy(
            wqkv.at[:, pl.ds(pl.multiple_of(1536 + 256 * core, 256), 256)],
            ZW.at[me, :, pl.ds(256, 256)],
            s_loc.at[2],
        ),
        pltpu.make_async_copy(
            wqkv.at[:, pl.ds(pl.multiple_of(512 * core, 512), 512)], ZQ.at[me], s_loc.at[3]
        ),
        pltpu.make_async_copy(
            wout.at[:, pl.ds(pl.multiple_of(1152 * core, 128), 1152)], ZO.at[me], s_loc.at[4]
        ),
        pltpu.make_async_copy(seg, SEGW.at[16 + me], s_loc.at[5]),
    ]
    for copy in local:
        copy.start()

    pl.semaphore_wait(barrier, 23)

    def z_copies(p, c, to):
        if p == 0:
            src, dst = wqkv.at[:, pl.ds(pl.multiple_of(1024 + 256 * c, 256), 256)], ZW.at[me, :, pl.ds(0, 256)]
        elif p == 1:
            src, dst = wqkv.at[:, pl.ds(pl.multiple_of(1536 + 256 * c, 256), 256)], ZW.at[me, :, pl.ds(256, 256)]
        elif p == 2:
            src, dst = wqkv.at[:, pl.ds(pl.multiple_of(512 * c, 512), 512)], ZQ.at[me]
        else:
            src, dst = wout.at[:, pl.ds(pl.multiple_of(1152 * c, 128), 1152)], ZO.at[me]
        return rc(src, dst, s_z.at[p], r_z.at[p], to)

    def z_send(*pieces):
        for d in (2, 6, 1, 7):
            for c in (0, 1):
                for p in pieces:
                    z_copies(p, c, z_dev(d, c)).start()

        for p in pieces:
            z_copies(p, other, mate).start()

    def z_near(p):
        if p == 0:
            return ZW.at[pl.ds(0, 9), :, pl.ds(0, 256)]
        if p == 1:
            return ZW.at[pl.ds(0, 9), :, pl.ds(256, 256)]
        return ZQ.at[pl.ds(0, 9)] if p == 2 else ZO.at[pl.ds(0, 9)]

    def z_got(*pieces):
        for p in pieces:
            got(z_near(p), r_z.at[p])

    def z_forward(k):
        Z = (ZW, ZQ, ZO)[k]

        def on(d, to, cols=None):
            slots = pl.ds(lax.rem(z + d, 8) * 2, 2)
            ref = Z.at[slots] if cols is None else Z.at[slots, :, cols]
            rc(ref, ref, s_f.at[k], r_f.at[k], z_dev(to, core)).start()

        on(1, 6)
        on(7, 2)
        if k == 2:
            on(2, 6)
        else:
            on(2, 6, pl.ds(0, 256))
            on(6, 2, pl.ds(256, 256))

    def z_far(k):
        return (ZW, ZQ, ZO)[k].at[pl.ds(0, 6)]

    def seg_copy(to):
        return rc(seg, SEGW.at[16 + me], s_m.at[5], r_m.at[5], to)

    z_send(0, 1)
    send(hid, H.at[own], s_m.at[1], r_m.at[1], mate)

    @pl.loop(1, 8)
    def _(d):
        for c in (0, 1):
            seg_copy(z_dev(d, c)).start()

    seg_copy(mate).start()

    def norm_rows(first):
        @pl.loop(0, TOK // 64)
        def _(i):
            rows = pl.ds(pl.multiple_of(first + i * 64, 64), 64)
            v = H[rows, :].astype(F32)
            v = v * lax.rsqrt(jnp.mean(v * v, axis=-1, keepdims=True) + EPS) * pre[...]
            v = v.astype(BF)
            N[0, rows, :] = v[:, : D // 2]
            N[1, rows, :] = v[:, D // 2 :]

    for i in range(D // 128):
        pre[:, pl.ds(128 * i, 128)] = pre18[pl.ds(i, 1), :]
        post[:, pl.ds(128 * i, 128)] = post18[pl.ds(i, 1), :]
    local[0].wait()
    norm_rows(core * TOK)
    theirs = pl.ds(pl.multiple_of(other * TOK, TOK), TOK)
    got(H.at[theirs], r_m.at[1])
    norm_rows(other * TOK)

    @pl.loop(0, CHIP // 64)
    def _(i):
        rows = pl.ds(pl.multiple_of(i * 64, 64), 64)
        places = lax.div(seq, 2) * CHIP + i * 64 + lax.broadcasted_iota(I32, (64, HEAD // 2), 0)
        angles = places.astype(F32) * inverse[...]
        cos[rows, :] = jnp.cos(angles)
        sin[rows, :] = jnp.sin(angles)

    def part(s, yy, half, xx=xl):
        ln = xx * 4 + yy
        n = OROWS if s == 2 else LROWS
        first, size = (0, n) if half is None else (half * (n // 2), n // 2)
        rows = pl.ds(pl.multiple_of(ln * n + first, 16), size)
        if s == 2:
            return WO.at[core, rows, :]
        return W.at[rows, pl.ds(512 * s, 512)]

    def to_y(s, yy, half, to, k):
        ref = part(s, yy, half)
        rc(ref, ref, s_y.at[s], r_y.at[s, k], to).start()

    meet = jnp.where((lax.rem(y, 3) == 0) & (lax.rem(z, 7) == 0), 1, 0)
    x0_out = dev(at_line(1 - xl, y), bat + meet * (1 - 2 * bat))

    def to_x(s, yy, half):
        ref = part(s, yy, half)
        if s < 2:
            rc(ref, ref, s_x.at[s], r_x.at[s], x1 if half else x0).start()
        else:
            rc(ref, ref, s_x.at[s], r_x.at[2 + yy], x1 if half else x0_out).start()
            rc(ref, ref, s_m.at[3], r_m.at[3], mate).start()

    def across(yy):
        ref = part(2, yy, None, 1 - xl)
        got(ref, r_x.at[2 + yy])
        rc(ref, ref, s_m.at[3], r_m.at[3], mate).start()

    def stage1_up(s):
        to_y(s, y, 0, up, 0)
        to_y(s, y, 1, up, 1)

    def stage1(s):
        to_y(s, y, 1, down, 3)
        to_y(s, y, 0, down, 2)
        to_x(s, y, 0)
        to_x(s, y, 1)

    def from_below(s, half):
        got(part(s, ym, half), r_y.at[s, half])
        if s == 0 and half == 0:
            to_y(s, ym, 0, up, 4)
        to_x(s, ym, half)

    def from_above(s, half):
        got(part(s, yp, half), r_y.at[s, 2 + half])
        if s > 0 or half == 1:
            to_y(s, yp, half, down, 4 + half)
        to_x(s, yp, half)

    def stage2_up(s):
        from_below(s, 0)
        from_below(s, 1)

    def stage2(s):
        from_above(s, 1)
        from_above(s, 0)

    def from_second(s, half):
        got(part(s, y2, half), r_y.at[s, 4 + half])
        to_x(s, y2, half)

    def stage3(s):
        from_second(s, 0)
        from_second(s, 1)

    def stage4(s):
        first = pl.multiple_of((1 - xl) * (D // 2), 16)
        got(W.at[pl.ds(first, D // 2), pl.ds(512 * s, 512)], r_x.at[s])

    def streams_gone(s):
        n = OROWS if s == 2 else LROWS
        for rows, sem in ((3 * n, s_y.at[s]), (4 * n, s_x.at[s])):
            if s == 2:
                gone(WO.at[core, pl.ds(0, rows), :], sem)
            else:
                gone(W.at[pl.ds(0, rows), pl.ds(512 * s, 512)], sem)

    def repack(Z, col):
        for j in range(16):
            FS[pl.ds(18 * j, 18), :] = Z[j].astype(F32)
        W[pl.ds(pl.multiple_of(line * LROWS, 16), LROWS), pl.ds(col, 512)] = FS[...].astype(BF)

    z_got(0, 1)
    z_forward(0)
    got(z_far(0), r_f.at[0])
    local[1].wait()
    local[2].wait()
    repack(ZW, 0)
    stage1_up(0)
    stage1(0)
    z_send(2)
    from_below(0, 0)
    from_above(0, 1)
    z_got(2)
    z_forward(1)
    from_below(0, 1)
    from_above(0, 0)
    z_send(3)
    stage3(0)
    got(z_far(1), r_f.at[1])
    local[3].wait()
    repack(ZQ, 512)
    stage1_up(1)
    stage1(1)

    def project_half(col, xx, add, i):
        rows = pl.ds(i * TOK, TOK)
        w = W[pl.ds(pl.multiple_of(xx * (D // 2), 16), D // 2), pl.ds(col, 512)]
        term = jnp.dot(N[xx, rows, :], w, preferred_element_type=F32)
        ACC[rows, :] = ACC[rows, :] + term if add else term

    def project(col, xx, add):
        for i in (0, 1):
            project_half(col, xx, add, i)

    def turned(rows, col):
        a, b = ACC[rows, pl.ds(col, 128)], ACC[rows, pl.ds(col + 128, 128)]
        c, s = cos[rows, :], sin[rows, :]
        return (a * c - b * s).astype(BF), (b * c + a * s).astype(BF)

    project(0, xl, False)

    got(SEGW.at[pl.ds(16, 15)], r_m.at[5])
    local[5].wait()
    send(SEGW.at[pl.ds(16, 16)], SEGW.at[pl.ds(0, 16)], s_m.at[2], r_m.at[2], nxt8)
    for half in (0, 1):
        row = SEGW[16 + 2 * z + half].astype(F32)
        QS[pl.ds(half * TOK, TOK), :] = jnp.broadcast_to(row, (TOK, TOK)).T

    z_got(3)
    z_forward(2)
    stage4(0)
    def own_block(half, buf):
        project_half(0, 1 - xl, True, half)
        rows = pl.ds(half * TOK, TOK)
        low, high = turned(rows, 0)
        buf[0, 0, :, pl.ds(0, 128)] = low
        buf[0, 0, :, pl.ds(128, 128)] = high
        buf[0, 1] = ACC[rows, pl.ds(256, 256)].astype(BF)

    def piece(buf, t, c):
        return buf.at[t, c // 2, pl.ds(c % 2 * 128, 128), :]

    def stop(buf, k, c):
        return buf.at[k, c // 2, pl.ds(c % 2 * 128, 128), :]

    def pass_on(buf, t, u, c, ss, rs, to):
        rc(piece(buf, t, c), piece(buf, u, c), ss, rs.at[u, c], to).start()

    def pass_a(j, c):
        around = (z == 7) & (core == 1)

        @pl.when(jnp.logical_not(around))
        def _():
            pass_on(A, j, j + 1, c, s_a.at[0], r_a, nxt)

        @pl.when(around)
        def _():
            rc(piece(A, j, c), stop(RA, j, c), s_a.at[0], r_d.at[j, c], nxt8).start()

    def pass_b(j, c):
        t = 9 - j
        around = (z == 0) & (core == 1)

        @pl.when(jnp.logical_not(around))
        def _():
            pass_on(B, t, t - 1, c, s_b.at[0], r_b, prv)

        @pl.when(around)
        def _():
            rc(piece(B, t, c), stop(RB, j - 1, c), s_b.at[0], r_d.at[j - 1, c], prv8).start()

    def take_a(e):
        j, c = divmod(e, 4)
        if 1 <= j <= 7:
            got(piece(A, j, c), r_a.at[j, c])
        if 1 <= j <= 6:
            pass_a(j, c)

    def take_b(e):
        j, c = divmod(e, 4)
        if 1 <= j <= 8:
            got(piece(B, 9 - j, c), r_b.at[9 - j, c])
        if 1 <= j <= 7:
            pass_b(j, c)

    def help_a(e):
        j, c = divmod(e, 4)
        if 0 <= j <= 6:
            ref = stop(RA, j, c)
            got(ref, r_d.at[j, c])
            rc(ref, piece(A, j + 1, c), s_d.at[0], r_a.at[j + 1, c], z0).start()

    def help_b(e):
        j, c = divmod(e, 4)
        if 1 <= j <= 7:
            ref = stop(RB, j - 1, c)
            got(ref, r_d.at[j - 1, c])
            rc(ref, piece(B, 8 - j, c), s_d.at[0], r_b.at[8 - j, c], z7).start()

    def relay(e):
        for c in (0, 1):
            @pl.when((z == 0) & (core == c))
            def _():
                take_b(e)
                if c:
                    help_b(e - LAGS[2])
                take_a(e - LAGS[c])

            @pl.when((z == 7) & (core == c))
            def _():
                take_a(e)
                if c:
                    help_a(e - LAGS[2])
                take_b(e - LAGS[c])

        @pl.when((z > 0) & (z < 4))
        def _():
            take_b(e)
            take_a(e)

        @pl.when((z > 3) & (z < 7))
        def _():
            take_a(e)
            take_b(e)

    own_block(1, B)
    for c in range(4):
        pass_on(B, 0, 8, c, s_b.at[1], r_b, nxt8)
    own_block(0, A)
    for c in range(4):
        pass_a(0, c)

    def attend(j, part):
        blocks = (
            ((A, 0, 0), (B, 0, 1)),
            *(((A, t, 0), (B, 9 - t, 1)) for t in range(1, 8)),
            ((B, 1, 1),),
            ((A, 8, 0),),
        )[j]
        docs, firsts = [], []
        for _, t, half in blocks:
            index = 16 + 2 * z + half - 2 * t
            shut = jnp.logical_and(index < 16, line == 0)
            docs.append(jnp.where(shut, -1.0, SEGW[index].astype(F32)))
            firsts.append(half * TOK - CHIP * t)

        @pl.loop(2 * part, 2 * part + 2, unroll=2)
        def _(r):
            rows = pl.ds(pl.multiple_of(r * TOK, TOK), TOK)
            tok = pl.multiple_of(lax.rem(r, 2) * TOK, TOK)
            queries, whose = QQ[rows, :], QS[pl.ds(tok, TOK), :]
            sums, mixed = None, None
            for (buf, t, _), doc, first in zip(blocks, docs, firsts):
                s = lax.dot_general(
                    queries, buf[t, 0], (((1,), (1,)), ((), ())), preferred_element_type=F32
                )
                w = jnp.exp2(jnp.tanh(s * (1.0 / (16.0 * CAP))) * (CAP * LOG2E))
                allowed = whose == doc
                if t in (0, 8):
                    behind = (
                        lax.broadcasted_iota(I32, (TOK, TOK), 0)
                        - lax.broadcasted_iota(I32, (TOK, TOK), 1)
                        + (tok - first)
                    )
                    allowed &= (behind >= 0) & (behind < WINDOW)
                w = jnp.where(allowed, w, 0.0)
                part_sum = w[:, :128] + w[:, 128:]
                term = jnp.dot(w.astype(BF), buf[t, 1], preferred_element_type=F32)
                sums = part_sum if sums is None else sums + part_sum
                mixed = term if mixed is None else mixed + term
            if j == 0:
                L[rows, :] = sums
                O[rows, :] = mixed
            else:
                L[rows, :] += sums
                O[rows, :] += mixed

    def relay_and(e):
        relay(e)
        for action in extra.get(e, ()):
            action()

    def relays(first, last):
        for e in range(first, last):
            relay_and(e)

    eighth = [lambda c=c: pass_on(A, 0, 8, c, s_a.at[1], r_a, nxt8) for c in range(4)]
    extra = {
        5: [lambda: from_above(1, 1)],
        7: [lambda: from_above(1, 0)],
        9: [lambda: from_below(1, 0)],
        10: [lambda: from_below(1, 1)],
        13: [lambda: from_second(1, 1), lambda: from_second(1, 0)],
        11: [lambda: to_y(2, y, 0, up, 0)],
        12: [lambda: to_y(2, y, 1, down, 3)],
        14: [lambda: to_y(2, y, 1, up, 1)],
        16: [lambda: to_y(2, y, 0, down, 2), lambda: to_x(2, y, 0), lambda: to_x(2, y, 1)],
        17: [eighth[0]],
        18: [lambda: from_above(2, 1)],
        19: [eighth[1]],
        20: [lambda: from_below(2, 0)],
        21: [eighth[2]],
        22: [lambda: from_above(2, 0)],
        23: [eighth[3]],
        24: [lambda: from_below(2, 1)],
        27: [lambda: from_second(2, 1)],
        29: [lambda: from_second(2, 0)],
        25: [lambda: across(y)],
        28: [lambda: across(yp)],
        30: [lambda: across(ym)],
        31: [lambda: [got(piece(A, 8, c), r_a.at[8, c]) for c in range(4)]],
        34: [lambda: across(y2)],
    }

    relays(3, 8)

    got(z_far(2), r_f.at[2])
    local[4].wait()
    for j in range(0, 16, 2):
        pair = jnp.concatenate([ZO[j].astype(F32), ZO[j + 1].astype(F32)], axis=0)
        WO[core, pl.ds(pl.multiple_of(line * OROWS + 8 * j, 16), 16), :] = pair.astype(BF)

    gone(SEGW.at[pl.ds(0, 15)], s_m.at[5])
    for p in range(4):
        gone(z_near(p), s_z.at[p])
    for k in range(3):
        gone(z_far(k), s_f.at[k])

    relays(8, 12)
    def queries_of(half):
        rows = pl.ds(half * TOK, TOK)
        for h in (0, 1):
            low, high = turned(rows, 256 * h)
            dst = pl.ds(h * CHIP + half * TOK, TOK)
            QQ[dst, pl.ds(0, 128)] = low
            QQ[dst, pl.ds(128, 128)] = high

    relays(12, Q_AT - 4)
    for half in (0, 1):
        relay_and(Q_AT - 4 + half)
        project_half(512, xl, False, half)
    relay_and(Q_AT - 2)
    stage4(1)
    project_half(512, 1 - xl, True, 0)
    queries_of(0)
    relay_and(Q_AT - 1)
    project_half(512, 1 - xl, True, 1)
    queries_of(1)
    got(SEGW.at[pl.ds(0, 16)], r_m.at[2])

    todo = [(j, p) for j in (0, 1, 2, 3, 4, 5, 6, 9, 7, 8) for p in (0, 1)]
    for e in range(Q_AT, 36 + LAG):
        relays(e, e + 1)
        for _ in range(1 if e % 2 else 2):
            if todo and (31 if todo[0][0] == 9 else 4 * todo[0][0] + 3 + LAG) <= e:
                attend(*todo.pop(0))
    for j, p in todo:
        attend(j, p)

    def attended(half, put):
        for h in (0, 1):
            rows = pl.ds(pl.multiple_of(h * CHIP + half * TOK, TOK), TOK)
            share = 1.0 / jnp.sum(L[rows, :], axis=-1, keepdims=True)
            put(h, (O[rows, :] * share).astype(BF))

    def put_other(h, value):
        SB[:, pl.ds(h * HEAD, HEAD)] = value

    def put_own(h, value):
        ATT[core, :, pl.ds(h * HEAD, HEAD)] = value

    attended(other, put_other)
    send(SB, ATT.at[core], s_m.at[4], r_m.at[4], mate)
    attended(core, put_own)
    got(WO.at[other], r_m.at[3])

    def branch(g, add):
        for c in (0, 1):
            cols = pl.ds(c * (D // 2), D // 2)
            weights = WO[c, pl.ds(pl.multiple_of(g * 512, 512), 512), :]
            term = jnp.dot(ATT[g], weights, preferred_element_type=F32)
            BR[:, cols] = BR[:, cols] + term if add else term

    branch(core, False)
    got(ATT.at[other], r_m.at[4])
    branch(other, True)

    @pl.loop(0, TOK // 32, unroll=2)
    def _(i):
        rows = pl.ds(pl.multiple_of(i * 32, 32), 32)
        v = BR[rows, :]
        v = v * lax.rsqrt(jnp.mean(v * v, axis=-1, keepdims=True) + EPS) * post[...]
        x = H[pl.ds(pl.multiple_of(core * TOK + i * 32, 32), 32), :].astype(F32)
        out[rows, :] = (x + v).astype(BF)

    for copy in sends:
        copy.wait_send()
    for buf, sem in ((A, s_a), (B, s_b)):
        gone(buf.at[pl.ds(0, 7)], sem.at[0])
        gone(buf.at[0], sem.at[1])
    @pl.when((lax.rem(z, 7) == 0) & (core == 1))
    def _():
        gone(A.at[pl.ds(0, 7)], s_d.at[0])

    for stream in range(3):
        streams_gone(stream)
    gone(WO.at[core], s_m.at[3])


def per_device(hidden_in, segment_ids, pre_gain, w_qkv, w_out, post_gain):
    inverse = np.float32(1.0) / np.float32(10000.0) ** (np.arange(HEAD // 2, dtype=np.float32) * 2 / HEAD)
    hbm = pl.BlockSpec(memory_space=pltpu.HBM)
    vmem = pl.BlockSpec(memory_space=pltpu.VMEM)
    dma = pltpu.SemaphoreType.DMA
    result = pl.pallas_call(
        kernel,
        out_shape=pltpu.VMEM((TOK, D), BF),
        in_specs=[hbm] * 4 + [vmem] * 3,
        out_specs=vmem,
        scratch_shapes=[
            pltpu.VMEM((CHIP, HEAD // 2), F32),
            pltpu.VMEM((CHIP, HEAD // 2), F32),
            pltpu.VMEM((1, D), F32),
            pltpu.VMEM((1, D), F32),
            pltpu.VMEM((CHIP, D), BF),
            pltpu.VMEM((2, CHIP, D // 2), BF),
            pltpu.VMEM((D, 1024), BF),
            pltpu.VMEM((2, 1024, D // 2), BF),
            pltpu.VMEM((16, 18, 512), BF),
            pltpu.VMEM((16, 18, 512), BF),
            pltpu.VMEM((16, 8, D // 2), BF),
            pltpu.VMEM((LROWS, 512), F32),
            pltpu.VMEM((CHIP, 512), F32),
            pltpu.VMEM((2 * CHIP, HEAD), BF),
            pltpu.VMEM((2 * CHIP, HEAD), F32),
            pltpu.VMEM((2 * CHIP, 128), F32),
            pltpu.VMEM((9, 2, TOK, HEAD), BF),
            pltpu.VMEM((9, 2, TOK, HEAD), BF),
            pltpu.VMEM((7, 2, TOK, HEAD), BF),
            pltpu.VMEM((7, 2, TOK, HEAD), BF),
            pltpu.VMEM((32, 1, TOK), I32),
            pltpu.VMEM((CHIP, TOK), F32),
            pltpu.VMEM((2, TOK, 512), BF),
            pltpu.VMEM((TOK, 512), BF),
            pltpu.VMEM((TOK, D), F32),
            dma((6,)),
            dma((4,)), dma((4,)),
            dma((3,)), dma((3,)),
            dma((3,)), dma((3, 6)),
            dma((3,)), dma((6,)),
            dma((2,)), dma((9, 4)),
            dma((2,)), dma((9, 4)),
            dma((1,)), dma((7, 4)),
            dma((6,)), dma((6,)),
        ],
        compiler_params=pltpu.CompilerParams(
            collective_id=0, has_side_effects=True, vmem_limit_bytes=60 * 1024 * 1024
        ),
    )(
        hidden_in[0],
        segment_ids,
        w_qkv,
        w_out,
        jnp.asarray(inverse.astype(np.float32).reshape(1, HEAD // 2)),
        pre_gain.reshape(D // 128, 128),
        post_gain.reshape(D // 128, 128),
    )
    return result[None]


def solution(mesh):
    placed = (P("batch", "seq", None), P("batch", "seq"), P(), P("seq", None), P("seq", None), P())
    return jax.shard_map(
        per_device, mesh=mesh, in_specs=placed, out_specs=P("batch", "seq", None), check_vma=False
    )
```
